512 devices in a mesh: head: 8 (over y_hi, core), blk: 64 (over z, y_lo, x).
Axes of the slice: x: 4, y: 8 (y_hi: 4, y_lo: 2; y = y_hi * 2 + y_lo), z: 8, core: 2. Of those that a mesh axis runs over, the one named last changes fastest.
Arguments:
- query_rows: bfloat16 [64, 144, 3072], P('blk', 'head'), may hold values from -6 to 6
- key_rows: bfloat16 [64, 144, 3072], P('blk', 'head'), may hold values from -6 to 6
- value_rows: bfloat16 [64, 144, 3072], P('blk', 'head'), may hold values from -6 to 6
- query_tangent: bfloat16 [64, 144, 3072], P('blk', 'head'), may hold values from -6 to 6
- key_tangent: bfloat16 [64, 144, 3072], P('blk', 'head'), may hold values from -6 to 6
- value_tangent: bfloat16 [64, 144, 3072], P('blk', 'head'), may hold values from -6 to 6
- query_gain: float32 [128], replicated, may hold values from 1 to 6
- key_gain: float32 [128], replicated, may hold values from 1 to 6
Outputs:
- attended: bfloat16 [64, 144, 3072], P('blk', 'head')
- attended_tangent: bfloat16 [64, 144, 3072], P('blk', 'head')
The draws below stay inside these ranges and needn't reach their ends.
All inputs are finite; a program needn't handle non-finite values.
Results may differ from the reference program's by a relative error of at most 0.014.
The reference program's roundings to bfloat16 on the way count: a program that leaves them out, or rounds other values in their place, can miss the bound.
Values may be sent and summed in bfloat16 or wider, within the bound.
No kernel may reach another device: no remote copies, remote signals or barrier semaphores. Data moves between devices by JAX's collectives and lax.ppermute only.
A program may use at most 64 MiB of HBM per device.

```python
import math
import jax
import jax.numpy as jnp
from jax import lax

HEADS = 24
HD = 128
D = 3072
TXT = 512
GRID_W = 64
GROUP = 16
ROWS = 144
IMAGES = 4
SEQ = 2304
BLOCKS = 64


def joint_pair(key):
    shape = (IMAGES, SEQ, D)
    key_values = jax.random.normal(jax.random.fold_in(key, 101), shape, jnp.float32)
    query_values = jax.random.normal(jax.random.fold_in(key, 102), shape, jnp.float32)

    def blocked(feature_field):
        feature_field = jnp.clip(feature_field, -6.0, 6.0).reshape(IMAGES, GROUP, ROWS, D)
        return feature_field.transpose(1, 0, 2, 3).reshape(GROUP * IMAGES, ROWS, D).astype(jnp.bfloat16)
    return (blocked(query_values), blocked(key_values))


def gain_draw(key):
    return jnp.exp(jax.random.uniform(key, (HD,), jnp.float32, 0.0, jnp.log(2.2)))


def draw_query_rows(key, part):
    return joint_pair(key)[0]


def draw_key_rows(key, part):
    return joint_pair(key)[1]


def draw_query_gain(key, part):
    return gain_draw(jax.random.fold_in(key, 201))


def draw_key_gain(key, part):
    return gain_draw(jax.random.fold_in(key, 202))


def level_of(own_key, extent, shards, least, top_value):
    factor_of = 1.0
    for dim, blocks in shards:
        heights = jax.random.uniform(jax.random.fold_in(jax.random.fold_in(own_key, 6), dim), (blocks,), jnp.float32, least / len(shards), top_value / len(shards))
        factor_of = factor_of * jnp.repeat(jnp.exp(heights), extent[dim] // blocks).reshape((-1,) + (1,) * (len(extent) - 1 - dim))
    return factor_of


def normal_values(own_key, dims, spread, bound, shards=(), held_as=jnp.bfloat16):
    loudness = level_of(own_key, dims, shards, -0.22, 0.18) if shards else 1.0
    values = jax.random.normal(own_key, dims, jnp.float32) * spread * loudness
    return jnp.minimum(jnp.maximum(values, -bound), bound).astype(held_as)


def setup_inputs(seed: int = 0) -> dict:
    key_of = jax.random.split(jax.random.key(seed), 9)
    query_rows = draw_query_rows(jax.random.fold_in(key_of[8], 71), 0)
    key_rows = draw_key_rows(jax.random.fold_in(key_of[8], 71), 0)
    value_rows = normal_values(key_of[2], (BLOCKS, ROWS, D), 1.0, 6.0, ((0, 64), (1, 8)))
    query_tangent = normal_values(key_of[3], (BLOCKS, ROWS, D), 1.0, 6.0, ((0, 64), (1, 8)))
    key_tangent = normal_values(key_of[4], (BLOCKS, ROWS, D), 1.0, 6.0, ((0, 64), (1, 8)))
    value_tangent = normal_values(key_of[5], (BLOCKS, ROWS, D), 1.0, 6.0, ((0, 64), (1, 8)))
    query_gain = draw_query_gain(jax.random.fold_in(key_of[8], 71), 0)
    key_gain = draw_key_gain(jax.random.fold_in(key_of[8], 71), 0)
    return {"query_rows": query_rows, "key_rows": key_rows, "value_rows": value_rows, "query_tangent": query_tangent, "key_tangent": key_tangent, "value_tangent": value_tangent, "query_gain": query_gain, "key_gain": key_gain}


EPSILON = 1e-06
THETA = 10000.0

def rotation(first, count, head_dim):
    block_offsets = first + jnp.arange(count, dtype=jnp.int32)
    is_image = block_offsets >= TXT
    patch = jnp.maximum(block_offsets - TXT, 0)
    row_id = jnp.where(is_image, patch // GRID_W, 0).astype(jnp.float32)
    column_id = jnp.where(is_image, patch % GRID_W, 0).astype(jnp.float32)
    leading = head_dim // 8
    lateral = (head_dim - leading) // 2
    exponent = jnp.arange(lateral // 2, dtype=jnp.float32) * (2.0 / lateral)
    frequency = jnp.exp(-math.log(THETA) * exponent)
    angles = jnp.concatenate([jnp.zeros((count, leading // 2), jnp.float32), row_id[:, None] * frequency[None, :], column_id[:, None] * frequency[None, :]], axis=1)
    angles = jnp.repeat(angles, 2, axis=1)
    return (jnp.cos(angles), jnp.sin(angles))

def rotation_partner(head_dim):
    across = jnp.arange(head_dim, dtype=jnp.int32)
    lower = across[:, None]
    upper = across[None, :]
    forward = ((upper == lower + 1) & (lower % 2 == 0)).astype(jnp.float32)
    backward = ((lower == upper + 1) & (upper % 2 == 0)).astype(jnp.float32)
    return forward - backward

def normalize(raw, tangent, gain, cosine, sine, partner):
    values = raw.astype(jnp.float32)
    motion = tangent.astype(jnp.float32)
    inverse = lax.rsqrt(lax.optimization_barrier(jnp.mean(values * values, axis=-1, keepdims=True)) + EPSILON)
    coupling = lax.optimization_barrier(jnp.mean(values * motion, axis=-1, keepdims=True))
    normed = values * inverse * gain
    normalized_tangent = gain * (motion * inverse - values * inverse * inverse * inverse * coupling)

    def rotate(feature_field):
        return feature_field * cosine + jnp.dot(feature_field, partner, precision=lax.Precision.HIGHEST) * sine
    return (rotate(normed).astype(jnp.bfloat16), rotate(normalized_tangent).astype(jnp.bfloat16))

def attend(item):
    query_hat, query_dot, key_hat, key_dot, value, value_dot = [feature_field.astype(jnp.float32) for feature_field in item]
    scale = 1.0 / math.sqrt(HD)
    logit_scores = jnp.dot(query_hat, key_hat.T, preferred_element_type=jnp.float32) * scale
    peak = lax.optimization_barrier(jnp.max(logit_scores, axis=1, keepdims=True))
    weights = jnp.exp(logit_scores - peak)
    total = lax.optimization_barrier(jnp.sum(weights, axis=1, keepdims=True))
    score_dot = (jnp.dot(query_dot, key_hat.T, preferred_element_type=jnp.float32) + jnp.dot(query_hat, key_dot.T, preferred_element_type=jnp.float32)) * scale
    product = weights * score_dot
    drift = lax.optimization_barrier(jnp.sum(product, axis=1, keepdims=True))
    low_weights = lax.optimization_barrier(weights.astype(jnp.bfloat16)).astype(jnp.float32)
    low_product = lax.optimization_barrier(product.astype(jnp.bfloat16)).astype(jnp.float32)
    summed = jnp.dot(low_weights, value, preferred_element_type=jnp.float32)
    summed_dot = jnp.dot(low_weights, value_dot, preferred_element_type=jnp.float32) + jnp.dot(low_product, value, preferred_element_type=jnp.float32)
    attention_output = (summed / total).astype(jnp.bfloat16)
    output_tangent = ((summed_dot - drift / total * summed) / total).astype(jnp.bfloat16)
    return (attention_output, output_tangent)

def reference(query_rows, key_rows, value_rows, query_tangent, key_tangent, value_tangent, query_gain, key_gain):

    def unblock(blocked):
        return blocked.reshape(GROUP, IMAGES, ROWS, HEADS, HD).transpose(1, 0, 2, 3, 4).reshape(IMAGES, SEQ, HEADS, HD)
    cosine, sine = rotation(0, SEQ, HD)
    cosine = cosine[None, :, None, :]
    sine = sine[None, :, None, :]
    partner = rotation_partner(HD)
    query_hat, query_dot = normalize(unblock(query_rows), unblock(query_tangent), query_gain, cosine, sine, partner)
    key_hat, key_dot = normalize(unblock(key_rows), unblock(key_tangent), key_gain, cosine, sine, partner)

    def per_head_split(feature_field):
        return feature_field.transpose(0, 2, 1, 3).reshape(IMAGES * HEADS, SEQ, HD)
    items = tuple((per_head_split(feature_field) for feature_field in (query_hat, query_dot, key_hat, key_dot, unblock(value_rows), unblock(value_tangent))))
    attention_output, output_tangent = lax.map(attend, items)

    def regroup_blocks(feature_field):
        feature_field = feature_field.reshape(IMAGES, HEADS, SEQ, HD).transpose(0, 2, 1, 3)
        feature_field = feature_field.reshape(IMAGES, GROUP, ROWS, HEADS * HD).transpose(1, 0, 2, 3)
        return feature_field.reshape(GROUP * IMAGES, ROWS, HEADS * HD)
    return (regroup_blocks(attention_output), regroup_blocks(output_tangent))
```

```python
import math

import jax
import jax.numpy as jnp
from jax import lax
from jax.experimental import pallas as pl
from jax.experimental.pallas import tpu as pltpu
from jax.sharding import Mesh
from jax.sharding import PartitionSpec as P

HEADS = 24
HD = 128
D = 3072
TXT = 512
GRID_W = 64
ROWS = 144
LOCAL = 18
MAIN = 16
SLOTS = 32
SRC_ROWS = 576
SEND = 112
BACK = 40
EPSILON = 1e-06
THETA = 10000.0
SCALE = 1.0 / math.sqrt(HD)
F32 = jnp.float32
BF16 = jnp.bfloat16

VMEM = pl.BlockSpec(memory_space=pltpu.VMEM)
SMEM = pl.BlockSpec(memory_space=pltpu.SMEM)


def slot_of(head):
    return (head % 3) * 8 + head // 3


def lanes(head):
    return slice(head * HD, (head + 1) * HD)


def one_hot(shape, column_of_row, valid):
    row = lax.broadcasted_iota(jnp.int32, shape, 0)
    column = lax.broadcasted_iota(jnp.int32, shape, 1)
    return jnp.where((column == column_of_row(row)) & valid(row), 1.0, 0.0).astype(BF16)


def prepare(first, query, key, value, query_t, key_t, value_t, query_gain, key_gain, out, tails):
    token = first[0] + lax.broadcasted_iota(jnp.int32, (LOCAL, HD), 0)
    lane = lax.broadcasted_iota(jnp.int32, (LOCAL, HD), 1)
    patch = jnp.maximum(token - TXT, 0)
    is_image = token >= TXT
    row_id = jnp.where(is_image, lax.shift_right_logical(patch, 6), 0).astype(F32)
    column_id = jnp.where(is_image, patch & (GRID_W - 1), 0).astype(F32)
    pair = lax.shift_right_logical(lane, 1)
    of_row = pair < 36
    step = jnp.where(of_row, pair - 8, pair - 36).astype(F32)
    frequency = jnp.exp(-math.log(THETA) * (step * (2.0 / 56.0)))
    angle = jnp.where(pair < 8, 0.0, jnp.where(of_row, row_id, column_id) * frequency)
    cosine = jnp.cos(angle)
    sine = jnp.sin(angle)
    even = (lane & 1) == 0
    sine_even = jnp.where(even, -sine, 0.0)
    sine_odd = jnp.where(even, 0.0, sine)

    def rotate(x):
        after = pltpu.roll(x, HD - 1, 1)
        before = pltpu.roll(x, 1, 1)
        return (x * cosine + after * sine_even + before * sine_odd).astype(BF16)

    def normalize(raw, tangent, gain):
        x = raw.astype(F32)
        u = tangent.astype(F32)
        inverse = lax.rsqrt(jnp.mean(x * x, axis=1, keepdims=True) + EPSILON)
        coupling = jnp.mean(x * u, axis=1, keepdims=True)
        xr = x * inverse
        normed = xr * gain
        dotted = gain * (u * inverse - xr * (inverse * inverse * coupling))
        return rotate(normed), rotate(dotted)

    tails[...] = jnp.zeros_like(tails)
    qg = query_gain[...]
    kg = key_gain[...]
    for head in range(HEADS):
        here = lanes(head)
        slot = slot_of(head)
        q_hat, q_dot = normalize(query[:, here], query_t[:, here], qg)
        k_hat, k_dot = normalize(key[:, here], key_t[:, here], kg)
        parts = (q_hat, q_dot, k_hat, k_dot, value[:, here], value_t[:, here])
        for t, part in enumerate(parts):
            out[slot, 16 * t : 16 * t + 16, :] = part[:MAIN]
            tails[16 * t : 16 * t + 2, here] = part[MAIN:]
    pick = one_hot((16, 96), lambda r: (r >> 1) * 16 + (r & 1), lambda r: r < 12)
    slab = jnp.dot(pick, tails[...], preferred_element_type=F32).astype(BF16)
    for head in range(HEADS):
        out[slot_of(head), 96:112, :] = slab[:, lanes(head)]
    for slot in range(HEADS, SLOTS):
        out[slot] = jnp.zeros((SEND, HD), BF16)


def repack(received, query_pair, key_value):
    places = ((query_pair, 128), (query_pair, 0)) + tuple((key_value, 128 * j) for j in range(4))
    for source in range(SLOTS):
        for t, (ref, at) in enumerate(places):
            ref[16 * source : 16 * source + 16, at : at + HD] = received[source, 16 * t : 16 * t + 16, :]
    slabs = received[:, 96:112, :].reshape(SLOTS * 16, HD)
    for t, (ref, at) in enumerate(places):
        pick = one_hot((64, 512), lambda r: (r >> 1) * 16 + 2 * t + (r & 1), lambda r: r >= 0)
        rest = jnp.dot(pick, slabs, preferred_element_type=F32).astype(BF16)
        ref[512:576, at : at + HD] = rest


TRANSPOSED = (((1,), (1,)), ((), ()))
BQ = 192


def attend(query_pair, kv0, kv1, kv2, kv3, out, attended, attended_t):
    blocks = (kv0, kv1, kv2, kv3)
    for b in range(SRC_ROWS // BQ):
        at = slice(b * BQ, (b + 1) * BQ)
        pair = query_pair[at, :]
        hat = query_pair[at, HD:]
        scores = [
            lax.dot_general(hat, kv[:, 0:HD], TRANSPOSED, preferred_element_type=F32) for kv in blocks
        ]
        peak = jnp.max(scores[0], axis=1, keepdims=True)
        for s in scores[1:]:
            peak = jnp.maximum(peak, jnp.max(s, axis=1, keepdims=True))
        total = drift = both = extra = 0.0
        for s, kv in zip(scores, blocks):
            weights = jnp.exp2((s - peak) * (SCALE * math.log2(math.e)))
            moved = lax.dot_general(pair, kv[:, 0 : 2 * HD], TRANSPOSED, preferred_element_type=F32)
            product = weights * (moved * SCALE)
            total = total + jnp.sum(weights, axis=1, keepdims=True)
            drift = drift + jnp.sum(product, axis=1, keepdims=True)
            both = both + jnp.dot(
                weights.astype(BF16), kv[:, 2 * HD : 4 * HD], preferred_element_type=F32
            )
            extra = extra + jnp.dot(
                product.astype(BF16), kv[:, 2 * HD : 3 * HD], preferred_element_type=F32
            )
        summed = both[:, :HD]
        summed_dot = both[:, HD:] + extra
        attended[at, :] = (summed / total).astype(BF16)
        attended_t[at, :] = ((summed_dot - drift / total * summed) / total).astype(BF16)
    for source in range(SLOTS):
        at = slice(16 * source, 16 * source + 16)
        out[source, 0:16, :] = attended[at, :]
        out[source, 16:32, :] = attended_t[at, :]
    rest = jnp.concatenate([attended[512:576, :], attended_t[512:576, :]], axis=0)
    pick = one_hot(
        (256, 128),
        lambda r: (r >> 3) * 2 + (r & 1) + jnp.where((r & 2) > 0, 64, 0),
        lambda r: (r & 7) < 4,
    )
    slabs = jnp.dot(pick, rest, preferred_element_type=F32).astype(BF16)
    out[:, 32:40, :] = slabs.reshape(SLOTS, 8, HD)


def unpack(received, attended, attended_t, tails):
    tails[...] = jnp.zeros_like(tails)
    for head in range(HEADS):
        slot = slot_of(head)
        here = lanes(head)
        attended[0:16, here] = received[slot, 0:16, :]
        attended_t[0:16, here] = received[slot, 16:32, :]
        tails[0:8, here] = received[slot, 32:40, :]
    pick = one_hot((16, 16), lambda r: jnp.where(r < 8, r, r - 6), lambda r: (r & 7) < 2)
    rest = jnp.dot(pick, tails[...], preferred_element_type=F32)
    attended[16:18, :] = rest[0:2].astype(BF16)
    attended_t[16:18, :] = rest[8:10].astype(BF16)


def local(query, key, value, query_t, key_t, value_t, query_gain, key_gain):
    place = lax.axis_index("z") * 2 + lax.axis_index("ylo")
    share = lax.axis_index("yhi") * 2 + lax.axis_index("core")
    first = (place * ROWS + share * LOCAL).reshape(1)
    rows = [a.reshape(LOCAL, D) for a in (query, key, value, query_t, key_t, value_t)]
    message = pl.pallas_call(
        prepare,
        out_shape=jax.ShapeDtypeStruct((SLOTS, SEND, HD), BF16),
        in_specs=[SMEM] + [VMEM] * 8,
        out_specs=VMEM,
        scratch_shapes=[pltpu.VMEM((96, D), BF16)],
        name="prepare",
    )(first, *rows, query_gain.reshape(1, HD), key_gain.reshape(1, HD))
    received = lax.all_to_all(message, ("yhi", "z"), 0, 0, tiled=True)
    query_pair, own = pl.pallas_call(
        repack,
        out_shape=(
            jax.ShapeDtypeStruct((SRC_ROWS, 2 * HD), BF16),
            jax.ShapeDtypeStruct((SRC_ROWS, 4 * HD), BF16),
        ),
        in_specs=[VMEM],
        out_specs=(VMEM, VMEM),
        name="repack",
    )(received)
    swap = [(0, 1), (1, 0)]
    across = lax.ppermute(own, "ylo", swap)
    beside = lax.ppermute(own, "core", swap)
    across_beside = lax.ppermute(across, "core", swap)
    message = pl.pallas_call(
        attend,
        out_shape=jax.ShapeDtypeStruct((SLOTS, BACK, HD), BF16),
        in_specs=[VMEM] * 5,
        out_specs=VMEM,
        scratch_shapes=[pltpu.VMEM((SRC_ROWS, HD), BF16)] * 2,
        name="attend",
    )(query_pair, own, beside, across, across_beside)
    received = lax.all_to_all(message, ("yhi", "z"), 0, 0, tiled=True)
    attended, attended_t = pl.pallas_call(
        unpack,
        out_shape=(jax.ShapeDtypeStruct((LOCAL, D), BF16),) * 2,
        in_specs=[VMEM],
        out_specs=(VMEM, VMEM),
        scratch_shapes=[pltpu.VMEM((16, D), BF16)],
        name="unpack",
    )(received)
    return attended.reshape(1, LOCAL, D), attended_t.reshape(1, LOCAL, D)


def solution(mesh):
    fine = Mesh(mesh.devices.reshape(4, 2, 8, 2, 4), ("yhi", "core", "z", "ylo", "x"))
    spec = P(("z", "ylo", "x"), ("yhi", "core"), None)
    return jax.shard_map(
        local,
        mesh=fine,
        in_specs=(spec,) * 6 + (P(), P()),
        out_specs=(spec, spec),
        check_vma=False,
    )
```

```python
import math

import jax
import jax.numpy as jnp
from jax import lax
from jax.experimental import pallas as pl
from jax.experimental.pallas import tpu as pltpu
from jax.sharding import Mesh
from jax.sharding import PartitionSpec as P

HEADS = 24
HD = 128
D = 3072
TXT = 512
GRID_W = 64
ROWS = 144
LOCAL = 18
MAIN = 16
SLOTS = 32
SRC_ROWS = 576
SEND = 112
BACK = 40
EPSILON = 1e-06
THETA = 10000.0
SCALE = 1.0 / math.sqrt(HD)
F32 = jnp.float32
BF16 = jnp.bfloat16

VMEM = pl.BlockSpec(memory_space=pltpu.VMEM)
SMEM = pl.BlockSpec(memory_space=pltpu.SMEM)


def slot_of(head):
    return (head % 3) * 8 + head // 3


def lanes(head):
    return slice(head * HD, (head + 1) * HD)


def one_hot(shape, column_of_row, valid):
    row = lax.broadcasted_iota(jnp.int32, shape, 0)
    column = lax.broadcasted_iota(jnp.int32, shape, 1)
    return jnp.where((column == column_of_row(row)) & valid(row), 1.0, 0.0).astype(BF16)


def prepare(first, query, key, value, query_t, key_t, value_t, query_gain, key_gain, out, tails):
    token = first[0] + lax.broadcasted_iota(jnp.int32, (LOCAL, HD), 0)
    lane = lax.broadcasted_iota(jnp.int32, (LOCAL, HD), 1)
    patch = jnp.maximum(token - TXT, 0)
    is_image = token >= TXT
    row_id = jnp.where(is_image, lax.shift_right_logical(patch, 6), 0).astype(F32)
    column_id = jnp.where(is_image, patch & (GRID_W - 1), 0).astype(F32)
    pair = lax.shift_right_logical(lane, 1)
    of_row = pair < 36
    step = jnp.where(of_row, pair - 8, pair - 36).astype(F32)
    frequency = jnp.exp(-math.log(THETA) * (step * (2.0 / 56.0)))
    angle = jnp.where(pair < 8, 0.0, jnp.where(of_row, row_id, column_id) * frequency)
    cosine = jnp.cos(angle)
    sine = jnp.sin(angle)
    even = (lane & 1) == 0
    sine_even = jnp.where(even, -sine, 0.0)
    sine_odd = jnp.where(even, 0.0, sine)

    def rotate(x):
        after = pltpu.roll(x, HD - 1, 1)
        before = pltpu.roll(x, 1, 1)
        return (x * cosine + after * sine_even + before * sine_odd).astype(BF16)

    def normalize(raw, tangent, gain):
        x = raw.astype(F32)
        u = tangent.astype(F32)
        inverse = lax.rsqrt(jnp.mean(x * x, axis=1, keepdims=True) + EPSILON)
        coupling = jnp.mean(x * u, axis=1, keepdims=True)
        xr = x * inverse
        normed = xr * gain
        dotted = gain * (u * inverse - xr * (inverse * inverse * coupling))
        return rotate(normed), rotate(dotted)

    tails[...] = jnp.zeros_like(tails)
    qg = query_gain[...]
    kg = key_gain[...]
    for head in range(HEADS):
        here = lanes(head)
        slot = slot_of(head)
        q_hat, q_dot = normalize(query[:, here], query_t[:, here], qg)
        k_hat, k_dot = normalize(key[:, here], key_t[:, here], kg)
        parts = (q_hat, q_dot, k_hat, k_dot, value[:, here], value_t[:, here])
        for t, part in enumerate(parts):
            out[slot, 16 * t : 16 * t + 16, :] = part[:MAIN]
            tails[16 * t : 16 * t + 2, here] = part[MAIN:]
    pick = one_hot((16, 96), lambda r: (r >> 1) * 16 + (r & 1), lambda r: r < 12)
    slab = jnp.dot(pick, tails[...], preferred_element_type=F32).astype(BF16)
    for head in range(HEADS):
        out[slot_of(head), 96:112, :] = slab[:, lanes(head)]
    for slot in range(HEADS, SLOTS):
        out[slot] = jnp.zeros((SEND, HD), BF16)


def repack(received, query_pair, key_value):
    places = ((query_pair, 128), (query_pair, 0)) + tuple((key_value, 128 * j) for j in range(4))
    for source in range(SLOTS):
        for t, (ref, at) in enumerate(places):
            ref[16 * source : 16 * source + 16, at : at + HD] = received[source, 16 * t : 16 * t + 16, :]
    slabs = received[:, 96:112, :].reshape(SLOTS * 16, HD)
    for t, (ref, at) in enumerate(places):
        pick = one_hot((64, 512), lambda r: (r >> 1) * 16 + 2 * t + (r & 1), lambda r: r >= 0)
        rest = jnp.dot(pick, slabs, preferred_element_type=F32).astype(BF16)
        ref[512:576, at : at + HD] = rest


TRANSPOSED = (((1,), (1,)), ((), ()))
BQ = 192


def absorb(query_pair, blocks, at, state):
    pair = query_pair[at, :]
    hat = query_pair[at, HD:]
    scores = [lax.dot_general(hat, kv[:, 0:HD], TRANSPOSED, preferred_element_type=F32) for kv in blocks]
    peak = None if state is None else state[0]
    for s in scores:
        top = jnp.max(s, axis=1, keepdims=True)
        peak = top if peak is None else jnp.maximum(peak, top)
    total = drift = both = extra = 0.0
    for s, kv in zip(scores, blocks):
        weights = jnp.exp2((s - peak) * (SCALE * math.log2(math.e)))
        moved = lax.dot_general(pair, kv[:, 0 : 2 * HD], TRANSPOSED, preferred_element_type=F32)
        product = weights * (moved * SCALE)
        total = total + jnp.sum(weights, axis=1, keepdims=True)
        drift = drift + jnp.sum(product, axis=1, keepdims=True)
        both = both + jnp.dot(weights.astype(BF16), kv[:, 2 * HD : 4 * HD], preferred_element_type=F32)
        extra = extra + jnp.dot(product.astype(BF16), kv[:, 2 * HD : 3 * HD], preferred_element_type=F32)
    summed = both[:, :HD]
    summed_dot = both[:, HD:] + extra
    if state is None:
        return peak, total, drift, summed, summed_dot
    rescale = jnp.exp2((state[0] - peak) * (SCALE * math.log2(math.e)))
    old = [part * rescale for part in state[1:]]
    return peak, old[0] + total, old[1] + drift, old[2] + summed, old[3] + summed_dot


QUERY_BLOCKS = [slice(b, b + BQ) for b in range(0, SRC_ROWS, BQ)]


def attend_first(query_pair, kv0, kv1, *state):
    for at in QUERY_BLOCKS:
        for ref, part in zip(state, absorb(query_pair, (kv0, kv1), at, None)):
            ref[at, :] = part


def attend_next(query_pair, kv, *states):
    before, after = states[:5], states[5:]
    for at in QUERY_BLOCKS:
        for ref, part in zip(after, absorb(query_pair, (kv,), at, [ref[at, :] for ref in before])):
            ref[at, :] = part


def attend_last(query_pair, kv, *rest):
    before, (out, attended, attended_t) = rest[:5], rest[5:]
    for at in QUERY_BLOCKS:
        state = absorb(query_pair, (kv,), at, [ref[at, :] for ref in before])
        _, total, drift, summed, summed_dot = state
        attended[at, :] = (summed / total).astype(BF16)
        attended_t[at, :] = ((summed_dot - drift / total * summed) / total).astype(BF16)
    for source in range(SLOTS):
        at = slice(16 * source, 16 * source + 16)
        out[source, 0:16, :] = attended[at, :]
        out[source, 16:32, :] = attended_t[at, :]
    tail = jnp.concatenate([attended[512:576, :], attended_t[512:576, :]], axis=0)
    pick = one_hot(
        (256, 128),
        lambda r: (r >> 3) * 2 + (r & 1) + jnp.where((r & 2) > 0, 64, 0),
        lambda r: (r & 7) < 4,
    )
    slabs = jnp.dot(pick, tail, preferred_element_type=F32).astype(BF16)
    out[:, 32:40, :] = slabs.reshape(SLOTS, 8, HD)


def unpack(received, attended, attended_t, tails):
    tails[...] = jnp.zeros_like(tails)
    for head in range(HEADS):
        slot = slot_of(head)
        here = lanes(head)
        attended[0:16, here] = received[slot, 0:16, :]
        attended_t[0:16, here] = received[slot, 16:32, :]
        tails[0:8, here] = received[slot, 32:40, :]
    pick = one_hot((16, 16), lambda r: jnp.where(r < 8, r, r - 6), lambda r: (r & 7) < 2)
    rest = jnp.dot(pick, tails[...], preferred_element_type=F32)
    attended[16:18, :] = rest[0:2].astype(BF16)
    attended_t[16:18, :] = rest[8:10].astype(BF16)


def call(kernel, outs, scratch=(), on_chip=True, kept=True, keys=0):
    make = pltpu.VMEM if kept else jax.ShapeDtypeStruct
    shapes = tuple(make(shape, dtype) for shape, dtype in outs)
    one = len(shapes) == 1

    def run(*args):
        if on_chip:
            specs = [VMEM] * len(args)
            args = [pltpu.with_memory_space_constraint(a, pltpu.VMEM) for a in args]
        else:
            specs = [SMEM] + [VMEM] * (len(args) - 1)
        return pl.pallas_call(
            kernel,
            out_shape=shapes[0] if one else shapes,
            in_specs=specs,
            out_specs=VMEM if one else (VMEM,) * len(shapes),
            scratch_shapes=list(scratch),
            cost_estimate=pl.CostEstimate(
                flops=16 * SRC_ROWS * HD * keys, transcendentals=SRC_ROWS * keys, bytes_accessed=10**6
            ),
            compiler_params=pltpu.CompilerParams(vmem_limit_bytes=24 * 2**20),
            name=kernel.__name__,
        )(*args)

    return run


def local(query, key, value, query_t, key_t, value_t, query_gain, key_gain):
    place = lax.axis_index("z") * 2 + lax.axis_index("ylo")
    share = lax.axis_index("yhi") * 2 + lax.axis_index("core")
    first = (place * ROWS + share * LOCAL).reshape(1)
    rows = [a.reshape(LOCAL, D) for a in (query, key, value, query_t, key_t, value_t)]
    message = call(prepare, [((SLOTS, SEND, HD), BF16)], [pltpu.VMEM((96, D), BF16)], on_chip=False)(
        first, *rows, query_gain.reshape(1, HD), key_gain.reshape(1, HD)
    )
    received = lax.all_to_all(message, ("yhi", "z"), 0, 0, tiled=True)
    query_pair, own = call(repack, [((SRC_ROWS, 2 * HD), BF16), ((SRC_ROWS, 4 * HD), BF16)])(received)
    swap = [(0, 1), (1, 0)]
    across = lax.ppermute(own, "ylo", swap)
    beside = lax.ppermute(own, "core", swap)
    state_shapes = [((SRC_ROWS, 1), F32)] * 3 + [((SRC_ROWS, HD), F32)] * 2
    state = call(attend_first, state_shapes, keys=2 * SRC_ROWS)(query_pair, own, beside)
    across, *state = lax.optimization_barrier((across, *state))
    across_beside = lax.ppermute(across, "core", swap)
    state = call(attend_next, state_shapes, keys=SRC_ROWS)(query_pair, across, *state)
    message = call(attend_last, [((SLOTS, BACK, HD), BF16)], [pltpu.VMEM((SRC_ROWS, HD), BF16)] * 2, keys=SRC_ROWS)(
        query_pair, across_beside, *state
    )
    received = lax.all_to_all(message, ("yhi", "z"), 0, 0, tiled=True)
    attended, attended_t = call(unpack, [((LOCAL, D), BF16)] * 2, [pltpu.VMEM((16, D), BF16)], kept=False)(
        received
    )
    return attended.reshape(1, LOCAL, D), attended_t.reshape(1, LOCAL, D)


def solution(mesh):
    fine = Mesh(mesh.devices.reshape(4, 2, 8, 2, 4), ("yhi", "core", "z", "ylo", "x"))
    spec = P(("z", "ylo", "x"), ("yhi", "core"), None)
    return jax.shard_map(
        local,
        mesh=fine,
        in_specs=(spec,) * 6 + (P(), P()),
        out_specs=(spec, spec),
        check_vma=False,
    )
```

```python
import math

import jax
import jax.numpy as jnp
from jax import lax
from jax.experimental import pallas as pl
from jax.experimental.pallas import tpu as pltpu
from jax.sharding import Mesh
from jax.sharding import PartitionSpec as P

HEADS = 24
HD = 128
D = 3072
TXT = 512
GRID_W = 64
ROWS = 144
LOCAL = 18
MAIN = 16
SLOTS = 32
SRC_ROWS = 576
EARLY = 320
SEND = 112
BACK = 40
EPSILON = 1e-06
THETA = 10000.0
SCALE = 1.0 / math.sqrt(HD)
F32 = jnp.float32
BF16 = jnp.bfloat16

VMEM = pl.BlockSpec(memory_space=pltpu.VMEM)
SMEM = pl.BlockSpec(memory_space=pltpu.SMEM)
HBM = pl.BlockSpec(memory_space=pltpu.HBM)


def slot_of(head):
    return (head % 3) * 8 + head // 3


def lanes(head):
    return slice(head * HD, (head + 1) * HD)


def one_hot(shape, column_of_row, valid):
    row = lax.broadcasted_iota(jnp.int32, shape, 0)
    column = lax.broadcasted_iota(jnp.int32, shape, 1)
    return jnp.where((column == column_of_row(row)) & valid(row), 1.0, 0.0).astype(BF16)


def prepare(first, *refs):
    sources, (out, tails), buffers, arrival = refs[:8], refs[8:10], refs[10:18], refs[18]
    copies = [
        pltpu.make_async_copy(source, buffer, arrival.at[i])
        for i, (source, buffer) in enumerate(zip(sources, buffers))
    ]
    for copy in copies:
        copy.start()
    query, key, value, query_t, key_t, value_t, query_gain, key_gain = buffers
    token = first[0] + lax.broadcasted_iota(jnp.int32, (LOCAL, HD), 0)
    lane = lax.broadcasted_iota(jnp.int32, (LOCAL, HD), 1)
    patch = jnp.maximum(token - TXT, 0)
    is_image = token >= TXT
    row_id = jnp.where(is_image, lax.shift_right_logical(patch, 6), 0).astype(F32)
    column_id = jnp.where(is_image, patch & (GRID_W - 1), 0).astype(F32)
    pair = lax.shift_right_logical(lane, 1)
    of_row = pair < 36
    step = jnp.where(of_row, pair - 8, pair - 36).astype(F32)
    frequency = jnp.exp(-math.log(THETA) * (step * (2.0 / 56.0)))
    angle = jnp.where(pair < 8, 0.0, jnp.where(of_row, row_id, column_id) * frequency)
    cosine = jnp.cos(angle)
    even = (lane & 1) == 0
    sine = jnp.where(even, -jnp.sin(angle), jnp.sin(angle))

    def turned(gain):
        wide = jnp.broadcast_to(gain, (LOCAL, HD))
        partner = jnp.where(even, pltpu.roll(wide, HD - 1, 1), pltpu.roll(wide, 1, 1))
        return wide * cosine, partner * sine

    exchange = one_hot((HD, HD), lambda r: r ^ 1, lambda r: r >= 0)

    def normalize(raw, tangent, own, other):
        x = raw.astype(F32)
        u = tangent.astype(F32)
        inverse = lax.rsqrt(jnp.mean(x * x, axis=1, keepdims=True) + EPSILON)
        coupling = jnp.mean(x * u, axis=1, keepdims=True)
        x_turned = x * own + jnp.dot(raw, exchange, preferred_element_type=F32) * other
        u_turned = u * own + jnp.dot(tangent, exchange, preferred_element_type=F32) * other
        dotted = u_turned * inverse - x_turned * (inverse * inverse * inverse * coupling)
        return (x_turned * inverse).astype(BF16), dotted.astype(BF16)

    tails[...] = jnp.zeros_like(tails)
    for slot in range(HEADS, SLOTS):
        out[slot] = jnp.zeros((SEND, HD), BF16)
    for copy in copies:
        copy.wait()
    of_query = turned(query_gain[...])
    of_key = turned(key_gain[...])
    for head in range(HEADS):
        here = lanes(head)
        slot = slot_of(head)
        q_hat, q_dot = normalize(query[:, here], query_t[:, here], *of_query)
        k_hat, k_dot = normalize(key[:, here], key_t[:, here], *of_key)
        parts = (q_hat, q_dot, k_hat, k_dot, value[:, here], value_t[:, here])
        for t, part in enumerate(parts):
            out[slot, 16 * t : 16 * t + 16, :] = part[:MAIN]
            tails[16 * t : 16 * t + 2, here] = part[MAIN:]
    pick = one_hot((16, 96), lambda r: (r >> 1) * 16 + (r & 1), lambda r: r < 12)
    slab = jnp.dot(pick, tails[...], preferred_element_type=F32).astype(BF16)
    for head in range(HEADS):
        out[slot_of(head), 96:112, :] = slab[:, lanes(head)]


def repack(received, query_pair, own, early, late):
    for source in range(SLOTS):
        row = 16 * source
        key_value, row_there = (early, row) if row < EARLY else (late, row - EARLY)
        for t, at in enumerate((128, 0, 0, 128, 256, 384)):
            part = received[source, 16 * t : 16 * t + 16, :]
            if t < 2:
                query_pair[row : row + 16, at : at + HD] = part
            else:
                own[row : row + 16, at : at + HD] = part
                key_value[row_there : row_there + 16, at : at + HD] = part
    slabs = received[:, 96:112, :].reshape(SLOTS * 16, HD)
    for t, at in enumerate((128, 0, 0, 128, 256, 384)):
        pick = one_hot((64, 512), lambda r: (r >> 1) * 16 + 2 * t + (r & 1), lambda r: r >= 0)
        part = jnp.dot(pick, slabs, preferred_element_type=F32).astype(BF16)
        if t < 2:
            query_pair[512:576, at : at + HD] = part
        else:
            own[512:576, at : at + HD] = part
            late[512 - EARLY : 576 - EARLY, at : at + HD] = part


TRANSPOSED = (((1,), (1,)), ((), ()))
BQ = 192


def absorb(query_pair, blocks, at, state):
    pair = query_pair[at, :]
    hat = query_pair[at, HD:]
    scores = [lax.dot_general(hat, kv[:, 0:HD], TRANSPOSED, preferred_element_type=F32) for kv in blocks]
    peak = None if state is None else state[0]
    for s in scores:
        top = jnp.max(s, axis=1, keepdims=True)
        peak = top if peak is None else jnp.maximum(peak, top)
    total = drift = both = extra = 0.0
    for s, kv in zip(scores, blocks):
        weights = jnp.exp2((s - peak) * (SCALE * math.log2(math.e)))
        moved = lax.dot_general(pair, kv[:, 0 : 2 * HD], TRANSPOSED, preferred_element_type=F32)
        product = weights * (moved * SCALE)
        total = total + jnp.sum(weights, axis=1, keepdims=True)
        drift = drift + jnp.sum(product, axis=1, keepdims=True)
        both = both + jnp.dot(weights.astype(BF16), kv[:, 2 * HD : 4 * HD], preferred_element_type=F32)
        extra = extra + jnp.dot(product.astype(BF16), kv[:, 2 * HD : 3 * HD], preferred_element_type=F32)
    summed = both[:, :HD]
    summed_dot = both[:, HD:] + extra
    if state is None:
        return peak, total, drift, summed, summed_dot
    rescale = jnp.exp2((state[0] - peak) * (SCALE * math.log2(math.e)))
    old = [part * rescale for part in state[1:]]
    return peak, old[0] + total, old[1] + drift, old[2] + summed, old[3] + summed_dot


QUERY_BLOCKS = [slice(b, b + BQ) for b in range(0, SRC_ROWS, BQ)]


def attend_first(query_pair, *rest):
    blocks, state = rest[:-5], rest[-5:]
    for at in QUERY_BLOCKS:
        for ref, part in zip(state, absorb(query_pair, blocks, at, None)):
            ref[at, :] = part


def attend_next(query_pair, *rest):
    blocks, before, after = rest[:-10], rest[-10:-5], rest[-5:]
    for at in QUERY_BLOCKS:
        for ref, part in zip(after, absorb(query_pair, blocks, at, [ref[at, :] for ref in before])):
            ref[at, :] = part


def attend_last(query_pair, kv, *rest):
    before, (out, attended, attended_t) = rest[:5], rest[5:]
    for at in QUERY_BLOCKS:
        state = absorb(query_pair, (kv,), at, [ref[at, :] for ref in before])
        _, total, drift, summed, summed_dot = state
        attended[at, :] = (summed / total).astype(BF16)
        attended_t[at, :] = ((summed_dot - drift / total * summed) / total).astype(BF16)
    for source in range(SLOTS):
        at = slice(16 * source, 16 * source + 16)
        out[source, 0:16, :] = attended[at, :]
        out[source, 16:32, :] = attended_t[at, :]
    tail = jnp.concatenate([attended[512:576, :], attended_t[512:576, :]], axis=0)
    pick = one_hot(
        (256, 128),
        lambda r: (r >> 3) * 2 + (r & 1) + jnp.where((r & 2) > 0, 64, 0),
        lambda r: (r & 7) < 4,
    )
    slabs = jnp.dot(pick, tail, preferred_element_type=F32).astype(BF16)
    out[:, 32:40, :] = slabs.reshape(SLOTS, 8, HD)


def unpack(received, attended, attended_t, tails):
    tails[...] = jnp.zeros_like(tails)
    for head in range(HEADS):
        slot = slot_of(head)
        here = lanes(head)
        attended[0:16, here] = received[slot, 0:16, :]
        attended_t[0:16, here] = received[slot, 16:32, :]
        tails[0:8, here] = received[slot, 32:40, :]
    pick = one_hot((16, 16), lambda r: jnp.where(r < 8, r, r - 6), lambda r: (r & 7) < 2)
    rest = jnp.dot(pick, tails[...], preferred_element_type=F32)
    attended[16:18, :] = rest[0:2].astype(BF16)
    attended_t[16:18, :] = rest[8:10].astype(BF16)


def call(kernel, outs, scratch=(), specs=None, kept=True, keys=0):
    make = pltpu.VMEM if kept else jax.ShapeDtypeStruct
    shapes = tuple(make(shape, dtype) for shape, dtype in outs)
    one = len(shapes) == 1

    def run(*args):
        places = specs or [VMEM] * len(args)
        args = [
            a if spec is SMEM else pltpu.with_memory_space_constraint(a, spec.memory_space)
            for a, spec in zip(args, places)
        ]
        return pl.pallas_call(
            kernel,
            out_shape=shapes[0] if one else shapes,
            in_specs=places,
            out_specs=VMEM if one else (VMEM,) * len(shapes),
            scratch_shapes=list(scratch),
            cost_estimate=pl.CostEstimate(
                flops=16 * SRC_ROWS * HD * keys, transcendentals=SRC_ROWS * keys, bytes_accessed=10**6
            ),
            compiler_params=pltpu.CompilerParams(vmem_limit_bytes=24 * 2**20),
        )(*args)

    return run


def local(query, key, value, query_t, key_t, value_t, query_gain, key_gain):
    place = lax.axis_index("z") * 2 + lax.axis_index("ylo")
    share = lax.axis_index("yhi") * 2 + lax.axis_index("core")
    first = (place * ROWS + share * LOCAL).reshape(1)
    rows = [a.reshape(LOCAL, D) for a in (query, key, value, query_t, key_t, value_t)]
    landing = [pltpu.VMEM((LOCAL, D), BF16)] * 6 + [pltpu.VMEM((1, HD), F32)] * 2
    landing.append(pltpu.SemaphoreType.DMA((8,)))
    message = call(
        prepare,
        [((SLOTS, SEND, HD), BF16)],
        [pltpu.VMEM((96, D), BF16)] + landing,
        specs=[SMEM] + [HBM] * 8,
    )(first, *rows, query_gain.reshape(1, HD), key_gain.reshape(1, HD))
    received = lax.all_to_all(message, ("yhi", "z"), 0, 0, tiled=True)
    query_pair, own, early, late = call(
        repack,
        [((SRC_ROWS, 2 * HD), BF16)] + [((n, 4 * HD), BF16) for n in (SRC_ROWS, EARLY, SRC_ROWS - EARLY)],
    )(received)
    state_shapes = [((SRC_ROWS, 1), F32)] * 3 + [((SRC_ROWS, HD), F32)] * 2

    def swapped(block, axis):
        return lax.ppermute(block, axis, [(0, 1), (1, 0)])

    early_across = swapped(early, "ylo")
    late_across = swapped(late, "ylo")
    own_beside = swapped(own, "core")
    state = call(attend_first, state_shapes, keys=2 * SRC_ROWS)(query_pair, own, own_beside)
    early_across, *state = lax.optimization_barrier((early_across, *state))
    early_both = swapped(early_across, "core")
    state = call(attend_next, state_shapes, keys=2 * EARLY)(query_pair, early_across, early_both, *state)
    late_across, *state = lax.optimization_barrier((late_across, *state))
    late_both = swapped(late_across, "core")
    state = call(attend_next, state_shapes, keys=SRC_ROWS - EARLY)(query_pair, late_across, *state)
    message = call(
        attend_last,
        [((SLOTS, BACK, HD), BF16)],
        [pltpu.VMEM((SRC_ROWS, HD), BF16)] * 2,
        keys=SRC_ROWS - EARLY,
    )(query_pair, late_both, *state)
    received = lax.all_to_all(message, ("yhi", "z"), 0, 0, tiled=True)
    attended, attended_t = call(unpack, [((LOCAL, D), BF16)] * 2, [pltpu.VMEM((16, D), BF16)], kept=False)(
        received
    )
    return attended.reshape(1, LOCAL, D), attended_t.reshape(1, LOCAL, D)


def solution(mesh):
    fine = Mesh(mesh.devices.reshape(4, 2, 8, 2, 4), ("yhi", "core", "z", "ylo", "x"))
    spec = P(("z", "ylo", "x"), ("yhi", "core"), None)
    return jax.shard_map(
        local,
        mesh=fine,
        in_specs=(spec,) * 6 + (P(), P()),
        out_specs=(spec, spec),
        check_vma=False,
    )
```

```python
import math

import jax
import jax.numpy as jnp
from jax import lax
from jax.experimental import pallas as pl
from jax.experimental.pallas import tpu as pltpu
from jax.sharding import Mesh
from jax.sharding import PartitionSpec as P

HEADS = 24
HD = 128
D = 3072
TXT = 512
GRID_W = 64
ROWS = 144
LOCAL = 18
MAIN = 16
CHIPS = 64
KEYS = 1152
QUERIES = 576
HALF = 9
SEND = 96
BACK = 24
EPSILON = 1e-06
THETA = 10000.0
SCALE = 1.0 / math.sqrt(HD)
F32 = jnp.float32
BF16 = jnp.bfloat16

VMEM = pl.BlockSpec(memory_space=pltpu.VMEM)
SMEM = pl.BlockSpec(memory_space=pltpu.SMEM)
HBM = pl.BlockSpec(memory_space=pltpu.HBM)


def chip_of(head, half):
    return (head % 3) * 16 + head // 3 * 2 + half


def lanes(head):
    return slice(head * HD, (head + 1) * HD)


def one_hot(shape, column_of_row, valid):
    row = lax.broadcasted_iota(jnp.int32, shape, 0)
    column = lax.broadcasted_iota(jnp.int32, shape, 1)
    return jnp.where((column == column_of_row(row)) & valid(row), 1.0, 0.0).astype(BF16)


def prepare(first, *refs):
    sources, (out, tails), buffers, arrival = refs[:8], refs[8:10], refs[10:18], refs[18]
    copies = [
        pltpu.make_async_copy(source, buffer, arrival.at[i])
        for i, (source, buffer) in enumerate(zip(sources, buffers))
    ]
    for copy in copies:
        copy.start()
    query, key, value, query_t, key_t, value_t, query_gain, key_gain = buffers
    token = first[0] + lax.broadcasted_iota(jnp.int32, (LOCAL, HD), 0)
    lane = lax.broadcasted_iota(jnp.int32, (LOCAL, HD), 1)
    patch = jnp.maximum(token - TXT, 0)
    is_image = token >= TXT
    row_id = jnp.where(is_image, lax.shift_right_logical(patch, 6), 0).astype(F32)
    column_id = jnp.where(is_image, patch & (GRID_W - 1), 0).astype(F32)
    pair = lax.shift_right_logical(lane, 1)
    of_row = pair < 36
    step = jnp.where(of_row, pair - 8, pair - 36).astype(F32)
    frequency = jnp.exp(-math.log(THETA) * (step * (2.0 / 56.0)))
    angle = jnp.where(pair < 8, 0.0, jnp.where(of_row, row_id, column_id) * frequency)
    cosine = jnp.cos(angle)
    even = (lane & 1) == 0
    sine = jnp.where(even, -jnp.sin(angle), jnp.sin(angle))

    def turned(gain):
        wide = jnp.broadcast_to(gain, (LOCAL, HD))
        partner = jnp.where(even, pltpu.roll(wide, HD - 1, 1), pltpu.roll(wide, 1, 1))
        return wide * cosine, partner * sine

    exchange = one_hot((HD, HD), lambda r: r ^ 1, lambda r: r >= 0)

    def normalize(raw, tangent, own, other):
        x = raw.astype(F32)
        u = tangent.astype(F32)
        inverse = lax.rsqrt(jnp.mean(x * x, axis=1, keepdims=True) + EPSILON)
        coupling = jnp.mean(x * u, axis=1, keepdims=True)
        x_turned = x * own + jnp.dot(raw, exchange, preferred_element_type=F32) * other
        u_turned = u * own + jnp.dot(tangent, exchange, preferred_element_type=F32) * other
        dotted = u_turned * inverse - x_turned * (inverse * inverse * inverse * coupling)
        return (x_turned * inverse).astype(BF16), dotted.astype(BF16)

    tails[...] = jnp.zeros_like(tails)
    for chip in range(2 * HEADS, CHIPS):
        out[chip] = jnp.zeros((SEND, HD), BF16)
    for copy in copies:
        copy.wait()
    of_query = turned(query_gain[...])
    of_key = turned(key_gain[...])
    for head in range(HEADS):
        here = lanes(head)
        q_hat, q_dot = normalize(query[:, here], query_t[:, here], *of_query)
        k_hat, k_dot = normalize(key[:, here], key_t[:, here], *of_key)
        tails[0:LOCAL, here] = q_hat
        tails[32 : 32 + LOCAL, here] = q_dot
        for t, part in enumerate((k_hat, k_dot, value[:, here], value_t[:, here])):
            for half in range(2):
                out[chip_of(head, half), 16 * t : 16 * t + 16, :] = part[:MAIN]
            tails[64 + 16 * t : 66 + 16 * t, here] = part[MAIN:]

    def column(r):
        half = r >> 5
        r = r & 31
        from_query = jnp.where(r < 8 + HALF, r - 8, r - 8 - HALF + 32) + HALF * half
        return jnp.where(r < 8, 64 + 16 * (r >> 1) + (r & 1), from_query)

    pick = one_hot((64, 128), column, lambda r: (r & 31) < 8 + 2 * HALF)
    slab = jnp.dot(pick, tails[...], preferred_element_type=F32).astype(BF16)
    for head in range(HEADS):
        for half in range(2):
            out[chip_of(head, half), 64:96, :] = slab[32 * half : 32 * half + 32, lanes(head)]


def repack(received, query_pair, own):
    for source in range(CHIPS):
        row = 16 * source
        for t in range(4):
            own[row : row + 16, HD * t : HD * t + HD] = received[source, 16 * t : 16 * t + 16, :]

    def column(r):
        query = r // HALF
        dotted = query >= 16
        from_query = (query & 15) * 32 + 8 + jnp.where(dotted, HALF, 0) + (r - query * HALF)
        rest = r - 288
        from_rest = ((rest & 31) >> 1) * 32 + (rest >> 5) * 2 + (rest & 1)
        return jnp.where(r < 288, from_query, from_rest)

    pick = one_hot((416, 512), column, lambda r: r >= 0)
    for two in range(2):
        slabs = [
            received[32 * two + 16 * g : 32 * two + 16 * g + 16, 64:96, :].reshape(512, HD) for g in range(2)
        ]
        picked = jnp.dot(pick, jnp.concatenate(slabs, axis=1), preferred_element_type=F32).astype(BF16)
        for g in range(2):
            group = 2 * two + g
            here = lanes(g)
            query_pair[144 * group : 144 * group + 144, HD:] = picked[0:144, here]
            query_pair[144 * group : 144 * group + 144, :HD] = picked[144:288, here]
            for t in range(4):
                rows = slice(1024 + 32 * group, 1024 + 32 * group + 32)
                own[rows, HD * t : HD * t + HD] = picked[288 + 32 * t : 320 + 32 * t, here]


TRANSPOSED = (((1,), (1,)), ((), ()))
BQ = 192


def absorb(query_pair, blocks, at, state):
    pair = query_pair[at, :]
    hat = query_pair[at, HD:]
    scores = [lax.dot_general(hat, kv[:, 0:HD], TRANSPOSED, preferred_element_type=F32) for kv in blocks]
    peak = None if state is None else state[0]
    for s in scores:
        top = jnp.max(s, axis=1, keepdims=True)
        peak = top if peak is None else jnp.maximum(peak, top)
    total = drift = both = extra = 0.0
    for s, kv in zip(scores, blocks):
        weights = jnp.exp2((s - peak) * (SCALE * math.log2(math.e)))
        moved = lax.dot_general(pair, kv[:, 0 : 2 * HD], TRANSPOSED, preferred_element_type=F32)
        product = weights * (moved * SCALE)
        total = total + jnp.sum(weights, axis=1, keepdims=True)
        drift = drift + jnp.sum(product, axis=1, keepdims=True)
        both = both + jnp.dot(weights.astype(BF16), kv[:, 2 * HD : 4 * HD], preferred_element_type=F32)
        extra = extra + jnp.dot(product.astype(BF16), kv[:, 2 * HD : 3 * HD], preferred_element_type=F32)
    summed = both[:, :HD]
    summed_dot = both[:, HD:] + extra
    if state is None:
        return peak, total, drift, summed, summed_dot
    rescale = jnp.exp2((state[0] - peak) * (SCALE * math.log2(math.e)))
    old = [part * rescale for part in state[1:]]
    return peak, old[0] + total, old[1] + drift, old[2] + summed, old[3] + summed_dot


QUERY_BLOCKS = [slice(b, b + BQ) for b in range(0, QUERIES, BQ)]


def attend_first(query_pair, *rest):
    blocks, state = rest[:-5], rest[-5:]
    for at in QUERY_BLOCKS:
        for ref, part in zip(state, absorb(query_pair, blocks, at, None)):
            ref[at, :] = part


def attend_last(query_pair, kv, *rest):
    before, (out, attended, attended_t) = rest[:5], rest[5:]
    for at in QUERY_BLOCKS:
        state = absorb(query_pair, (kv,), at, [ref[at, :] for ref in before])
        _, total, drift, summed, summed_dot = state
        attended[at, :] = (summed / total).astype(BF16)
        attended_t[at, :] = ((summed_dot - drift / total * summed) / total).astype(BF16)

    def column(r):
        source = r // BACK
        r = r - source * BACK
        return source * HALF + jnp.where(r < HALF, r, r - HALF + 144)

    pick = one_hot((16 * BACK, 288), column, lambda r: r % BACK < 2 * HALF)
    for two in range(2):
        sides = []
        for group in (2 * two, 2 * two + 1):
            at = slice(144 * group, 144 * group + 144)
            sides.append(jnp.concatenate([attended[at, :], attended_t[at, :]], axis=0))
        picked = jnp.dot(pick, jnp.concatenate(sides, axis=1), preferred_element_type=F32).astype(BF16)
        for g in range(2):
            sources = slice(16 * (2 * two + g), 16 * (2 * two + g) + 16)
            out[sources, :, :] = picked[:, lanes(g)].reshape(16, BACK, HD)


def unpack(received, attended, attended_t, both):
    both[...] = jnp.zeros_like(both)
    for head in range(HEADS):
        for half in range(2):
            both[32 * half : 32 * half + BACK, lanes(head)] = received[chip_of(head, half)]

    def from_message(r):
        row = r & 31
        half = jnp.where(row >= HALF, 1, 0)
        return 32 * half + row - HALF * half + jnp.where(r >= 32, HALF, 0)

    pick = one_hot((64, 64), from_message, lambda r: (r & 31) < LOCAL)
    rows = jnp.dot(pick, both[...], preferred_element_type=F32)
    attended[...] = rows[0:LOCAL].astype(BF16)
    attended_t[...] = rows[32 : 32 + LOCAL].astype(BF16)


def call(kernel, outs, scratch=(), specs=None, kept=True, keys=0):
    make = pltpu.VMEM if kept else jax.ShapeDtypeStruct
    shapes = tuple(make(shape, dtype) for shape, dtype in outs)
    one = len(shapes) == 1

    def run(*args):
        places = specs or [VMEM] * len(args)
        args = [
            a if spec is SMEM else pltpu.with_memory_space_constraint(a, spec.memory_space)
            for a, spec in zip(args, places)
        ]
        return pl.pallas_call(
            kernel,
            out_shape=shapes[0] if one else shapes,
            in_specs=places,
            out_specs=VMEM if one else (VMEM,) * len(shapes),
            scratch_shapes=list(scratch),
            cost_estimate=pl.CostEstimate(
                flops=16 * QUERIES * HD * keys, transcendentals=QUERIES * keys, bytes_accessed=10**6
            ),
            compiler_params=pltpu.CompilerParams(vmem_limit_bytes=24 * 2**20),
            name=kernel.__name__,
        )(*args)

    return run


def local(query, key, value, query_t, key_t, value_t, query_gain, key_gain):
    place = lax.axis_index("z") * 2 + lax.axis_index("ylo")
    share = lax.axis_index("yhi") * 2 + lax.axis_index("core")
    first = (place * ROWS + share * LOCAL).reshape(1)
    rows = [a.reshape(LOCAL, D) for a in (query, key, value, query_t, key_t, value_t)]
    landing = [pltpu.VMEM((LOCAL, D), BF16)] * 6 + [pltpu.VMEM((1, HD), F32)] * 2
    landing.append(pltpu.SemaphoreType.DMA((8,)))
    message = call(
        prepare,
        [((CHIPS, SEND, HD), BF16)],
        [pltpu.VMEM((128, D), BF16)] + landing,
        specs=[SMEM] + [HBM] * 8,
    )(first, *rows, query_gain.reshape(1, HD), key_gain.reshape(1, HD))
    received = lax.all_to_all(message, ("yhi", "z", "ylo"), 0, 0, tiled=True)
    query_pair, own = call(repack, [((QUERIES, 2 * HD), BF16), ((KEYS, 4 * HD), BF16)])(received)
    beside = lax.ppermute(own, "core", [(0, 1), (1, 0)])
    state_shapes = [((QUERIES, 1), F32)] * 3 + [((QUERIES, HD), F32)] * 2
    state = call(attend_first, state_shapes, keys=KEYS)(query_pair, own)
    message = call(
        attend_last, [((CHIPS, BACK, HD), BF16)], [pltpu.VMEM((QUERIES, HD), BF16)] * 2, keys=KEYS
    )(query_pair, beside, *state)
    received = lax.all_to_all(message, ("yhi", "z", "ylo"), 0, 0, tiled=True)
    attended, attended_t = call(unpack, [((LOCAL, D), BF16)] * 2, [pltpu.VMEM((64, D), BF16)], kept=False)(
        received
    )
    return attended.reshape(1, LOCAL, D), attended_t.reshape(1, LOCAL, D)


def solution(mesh):
    fine = Mesh(mesh.devices.reshape(4, 2, 8, 2, 4), ("yhi", "core", "z", "ylo", "x"))
    spec = P(("z", "ylo", "x"), ("yhi", "core"), None)
    return jax.shard_map(
        local,
        mesh=fine,
        in_specs=(spec,) * 6 + (P(), P()),
        out_specs=(spec, spec),
        check_vma=False,
    )
```

```python
import math

import jax
import jax.numpy as jnp
from jax import lax
from jax.experimental import pallas as pl
from jax.experimental.pallas import tpu as pltpu
from jax.sharding import Mesh
from jax.sharding import PartitionSpec as P

HEADS = 24
HD = 128
D = 3072
TXT = 512
GRID_W = 64
ROWS = 144
LOCAL = 18
CHIPS = 64
KEYS = 1152
QUERIES = 576
HALF = 9
SEND = 90
BACK = 18
EPSILON = 1e-06
THETA = 10000.0
SCALE = 1.0 / math.sqrt(HD)
F32 = jnp.float32
BF16 = jnp.bfloat16

VMEM = pl.BlockSpec(memory_space=pltpu.VMEM)
SMEM = pl.BlockSpec(memory_space=pltpu.SMEM)
HBM = pl.BlockSpec(memory_space=pltpu.HBM)


def chip_of(head, half):
    return (head % 3) * 16 + head // 3 * 2 + half


def lanes(head):
    return slice(head * HD, (head + 1) * HD)


def prepare(first, *refs):
    sources, out, buffers, arrival = refs[:8], refs[8], refs[9:17], refs[17]
    copies = [
        pltpu.make_async_copy(source, buffer, arrival.at[i])
        for i, (source, buffer) in enumerate(zip(sources, buffers))
    ]
    for copy in copies:
        copy.start()
    query, key, value, query_t, key_t, value_t, query_gain, key_gain = buffers
    token = first[0] + lax.broadcasted_iota(jnp.int32, (LOCAL, HD), 0)
    lane = lax.broadcasted_iota(jnp.int32, (LOCAL, HD), 1)
    patch = jnp.maximum(token - TXT, 0)
    is_image = token >= TXT
    row_id = jnp.where(is_image, lax.shift_right_logical(patch, 6), 0).astype(F32)
    column_id = jnp.where(is_image, patch & (GRID_W - 1), 0).astype(F32)
    pair = lax.shift_right_logical(lane, 1)
    of_row = pair < 36
    step = jnp.where(of_row, pair - 8, pair - 36).astype(F32)
    frequency = jnp.exp(-math.log(THETA) * (step * (2.0 / 56.0)))
    angle = jnp.where(pair < 8, 0.0, jnp.where(of_row, row_id, column_id) * frequency)
    cosine = jnp.cos(angle)
    even = (lane & 1) == 0
    sine = jnp.where(even, -jnp.sin(angle), jnp.sin(angle))

    def turned(gain):
        wide = jnp.broadcast_to(gain, (LOCAL, HD))
        partner = jnp.where(even, pltpu.roll(wide, HD - 1, 1), pltpu.roll(wide, 1, 1))
        return wide * cosine, partner * sine

    row = lax.broadcasted_iota(jnp.int32, (HD, HD), 0)
    column = lax.broadcasted_iota(jnp.int32, (HD, HD), 1)
    exchange = jnp.where((row ^ 1) == column, 1.0, 0.0).astype(BF16)

    def normalize(raw, tangent, own, other):
        x = raw.astype(F32)
        u = tangent.astype(F32)
        inverse = lax.rsqrt(jnp.mean(x * x, axis=1, keepdims=True) + EPSILON)
        coupling = jnp.mean(x * u, axis=1, keepdims=True)
        x_turned = x * own + jnp.dot(raw, exchange, preferred_element_type=F32) * other
        u_turned = u * own + jnp.dot(tangent, exchange, preferred_element_type=F32) * other
        dotted = u_turned * inverse - x_turned * (inverse * inverse * inverse * coupling)
        return x_turned * inverse, dotted

    idle = 2 * HEADS * SEND
    out[idle:, :] = jnp.zeros((CHIPS * SEND - idle, HD), BF16)
    for copy in copies:
        copy.wait()
    of_query = turned(query_gain[...])
    of_key = turned(key_gain[...])
    for head in range(HEADS):
        here = lanes(head)
        q_hat, q_dot = normalize(query[:, here], query_t[:, here], *of_query)
        k_hat, k_dot = normalize(key[:, here], key_t[:, here], *of_key)
        parts = (k_hat.astype(BF16), k_dot.astype(BF16), value[:, here], value_t[:, here])
        for half in range(2):
            at = chip_of(head, half) * SEND
            for t, part in enumerate(parts):
                out[at + LOCAL * t : at + LOCAL * t + LOCAL, :] = part
            ours = slice(HALF * half, HALF * half + HALF)
            queries = jnp.concatenate([q_hat[ours], q_dot[ours]], axis=0)
            out[at + 4 * LOCAL : at + SEND, :] = queries.astype(BF16)


def repack(received, query_pair, own):
    for source in range(CHIPS):
        at = source * SEND
        for t in range(4):
            own[LOCAL * source : LOCAL * source + LOCAL, HD * t : HD * t + HD] = received[
                at + LOCAL * t : at + LOCAL * t + LOCAL, :
            ]
    for source in range(0, CHIPS, 2):
        two = [received[s * SEND + 4 * LOCAL : s * SEND + SEND, :].astype(F32) for s in (source, source + 1)]
        rows = slice(HALF * source, HALF * source + LOCAL)
        query_pair[rows, HD:] = jnp.concatenate([part[:HALF] for part in two], axis=0).astype(BF16)
        query_pair[rows, :HD] = jnp.concatenate([part[HALF:] for part in two], axis=0).astype(BF16)


TRANSPOSED = (((1,), (1,)), ((), ()))
BQ = 192


def absorb(query_pair, blocks, at, state):
    pair = query_pair[at, :]
    hat = query_pair[at, HD:]
    scores = [lax.dot_general(hat, kv[:, 0:HD], TRANSPOSED, preferred_element_type=F32) for kv in blocks]
    peak = None if state is None else state[0]
    for s in scores:
        top = jnp.max(s, axis=1, keepdims=True)
        peak = top if peak is None else jnp.maximum(peak, top)
    total = drift = both = extra = 0.0
    for s, kv in zip(scores, blocks):
        weights = jnp.exp2((s - peak) * (SCALE * math.log2(math.e)))
        moved = lax.dot_general(pair, kv[:, 0 : 2 * HD], TRANSPOSED, preferred_element_type=F32)
        product = weights * (moved * SCALE)
        total = total + jnp.sum(weights, axis=1, keepdims=True)
        drift = drift + jnp.sum(product, axis=1, keepdims=True)
        both = both + jnp.dot(weights.astype(BF16), kv[:, 2 * HD : 4 * HD], preferred_element_type=F32)
        extra = extra + jnp.dot(product.astype(BF16), kv[:, 2 * HD : 3 * HD], preferred_element_type=F32)
    summed = both[:, :HD]
    summed_dot = both[:, HD:] + extra
    if state is None:
        return peak, total, drift, summed, summed_dot
    rescale = jnp.exp2((state[0] - peak) * (SCALE * math.log2(math.e)))
    old = [part * rescale for part in state[1:]]
    return peak, old[0] + total, old[1] + drift, old[2] + summed, old[3] + summed_dot


QUERY_BLOCKS = [slice(b, b + BQ) for b in range(0, QUERIES, BQ)]


def attend_first(query_pair, *rest):
    blocks, state = rest[:-5], rest[-5:]
    for at in QUERY_BLOCKS:
        for ref, part in zip(state, absorb(query_pair, blocks, at, None)):
            ref[at, :] = part


def attend_last(query_pair, kv, *rest):
    before, (out, attended, attended_t) = rest[:5], rest[5:]
    for at in QUERY_BLOCKS:
        state = absorb(query_pair, (kv,), at, [ref[at, :] for ref in before])
        _, total, drift, summed, summed_dot = state
        attended[at, :] = summed / total
        attended_t[at, :] = (summed_dot - drift / total * summed) / total
    for source in range(CHIPS):
        rows = slice(HALF * source, HALF * source + HALF)
        both = jnp.concatenate([attended[rows, :], attended_t[rows, :]], axis=0)
        out[BACK * source : BACK * source + BACK, :] = both.astype(BF16)


def unpack(received, attended, attended_t):
    for head in range(HEADS):
        halves = []
        for half in range(2):
            at = chip_of(head, half) * BACK
            halves.append(received[at : at + BACK, :].astype(F32))
        here = lanes(head)
        attended[:, here] = jnp.concatenate([part[:HALF] for part in halves], axis=0).astype(BF16)
        attended_t[:, here] = jnp.concatenate([part[HALF:] for part in halves], axis=0).astype(BF16)


def call(kernel, outs, scratch=(), specs=None, kept=True, keys=0):
    make = pltpu.VMEM if kept else jax.ShapeDtypeStruct
    shapes = tuple(make(shape, dtype) for shape, dtype in outs)
    one = len(shapes) == 1

    def run(*args):
        places = specs or [VMEM] * len(args)
        args = [
            a if spec is SMEM else pltpu.with_memory_space_constraint(a, spec.memory_space)
            for a, spec in zip(args, places)
        ]
        return pl.pallas_call(
            kernel,
            out_shape=shapes[0] if one else shapes,
            in_specs=places,
            out_specs=VMEM if one else (VMEM,) * len(shapes),
            scratch_shapes=list(scratch),
            cost_estimate=pl.CostEstimate(
                flops=16 * QUERIES * HD * keys, transcendentals=QUERIES * keys, bytes_accessed=10**6
            ),
            compiler_params=pltpu.CompilerParams(vmem_limit_bytes=24 * 2**20),
            name=kernel.__name__,
        )(*args)

    return run


def exchanged(message, rows):
    pairs = message.reshape(CHIPS, rows // 2, 2, HD)
    pairs = lax.all_to_all(pairs, ("yhi", "z", "ylo"), 0, 0, tiled=True)
    return pairs.reshape(CHIPS * rows, HD)


def local(query, key, value, query_t, key_t, value_t, query_gain, key_gain):
    place = lax.axis_index("z") * 2 + lax.axis_index("ylo")
    share = lax.axis_index("yhi") * 2 + lax.axis_index("core")
    first = (place * ROWS + share * LOCAL).reshape(1)
    rows = [a.reshape(LOCAL, D) for a in (query, key, value, query_t, key_t, value_t)]
    landing = [pltpu.VMEM((LOCAL, D), BF16)] * 6 + [pltpu.VMEM((1, HD), F32)] * 2
    landing.append(pltpu.SemaphoreType.DMA((8,)))
    message = call(
        prepare,
        [((CHIPS * SEND, HD), BF16)],
        landing,
        specs=[SMEM] + [HBM] * 8,
    )(first, *rows, query_gain.reshape(1, HD), key_gain.reshape(1, HD))
    received = exchanged(message, SEND)
    query_pair, own = call(repack, [((QUERIES, 2 * HD), BF16), ((KEYS, 4 * HD), BF16)])(received)
    beside = lax.ppermute(own, "core", [(0, 1), (1, 0)])
    state_shapes = [((QUERIES, 1), F32)] * 3 + [((QUERIES, HD), F32)] * 2
    state = call(attend_first, state_shapes, keys=KEYS)(query_pair, own)
    message = call(
        attend_last, [((CHIPS * BACK, HD), BF16)], [pltpu.VMEM((QUERIES, HD), F32)] * 2, keys=KEYS
    )(query_pair, beside, *state)
    received = exchanged(message, BACK)
    attended, attended_t = call(unpack, [((LOCAL, D), BF16)] * 2, kept=False)(received)
    return attended.reshape(1, LOCAL, D), attended_t.reshape(1, LOCAL, D)


def solution(mesh):
    fine = Mesh(mesh.devices.reshape(4, 2, 8, 2, 4), ("yhi", "core", "z", "ylo", "x"))
    spec = P(("z", "ylo", "x"), ("yhi", "core"), None)
    return jax.shard_map(
        local,
        mesh=fine,
        in_specs=(spec,) * 6 + (P(), P()),
        out_specs=(spec, spec),
        check_vma=False,
    )
```

```python
import math

import jax
import jax.numpy as jnp
from jax import lax
from jax.experimental import pallas as pl
from jax.experimental.pallas import tpu as pltpu
from jax.sharding import Mesh
from jax.sharding import PartitionSpec as P

HEADS = 24
HD = 128
D = 3072
TXT = 512
GRID_W = 64
ROWS = 144
LOCAL = 18
CHIPS = 64
KEYS = 1152
QUERIES = 576
HALF = 9
SEND = 90
BACK = 18
EPSILON = 1e-06
THETA = 10000.0
SCALE = 1.0 / math.sqrt(HD)
F32 = jnp.float32
BF16 = jnp.bfloat16

VMEM = pl.BlockSpec(memory_space=pltpu.VMEM)
SMEM = pl.BlockSpec(memory_space=pltpu.SMEM)
HBM = pl.BlockSpec(memory_space=pltpu.HBM)


def chip_of(head, half):
    return (head % 3) * 16 + head // 3 * 2 + half


def lanes(head):
    return slice(head * HD, (head + 1) * HD)


def prepare(first, *refs):
    sources, out, buffers, arrival = refs[:8], refs[8], refs[9:17], refs[17]
    copies = [
        pltpu.make_async_copy(source, buffer, arrival.at[i])
        for i, (source, buffer) in enumerate(zip(sources, buffers))
    ]
    for copy in copies:
        copy.start()
    query, key, value, query_t, key_t, value_t, query_gain, key_gain = buffers
    token = first[0] + lax.broadcasted_iota(jnp.int32, (LOCAL, HD), 0)
    lane = lax.broadcasted_iota(jnp.int32, (LOCAL, HD), 1)
    patch = jnp.maximum(token - TXT, 0)
    is_image = token >= TXT
    row_id = jnp.where(is_image, lax.shift_right_logical(patch, 6), 0).astype(F32)
    column_id = jnp.where(is_image, patch & (GRID_W - 1), 0).astype(F32)
    pair = lax.shift_right_logical(lane, 1)
    of_row = pair < 36
    step = jnp.where(of_row, pair - 8, pair - 36).astype(F32)
    frequency = jnp.exp(-math.log(THETA) * (step * (2.0 / 56.0)))
    angle = jnp.where(pair < 8, 0.0, jnp.where(of_row, row_id, column_id) * frequency)
    cosine = jnp.cos(angle)
    even = (lane & 1) == 0
    sine = jnp.where(even, -jnp.sin(angle), jnp.sin(angle))

    def turned(gain):
        wide = jnp.broadcast_to(gain, (LOCAL, HD))
        partner = jnp.where(even, pltpu.roll(wide, HD - 1, 1), pltpu.roll(wide, 1, 1))
        return wide * cosine, partner * sine

    row = lax.broadcasted_iota(jnp.int32, (HD, HD), 0)
    column = lax.broadcasted_iota(jnp.int32, (HD, HD), 1)
    exchange = jnp.where((row ^ 1) == column, 1.0, 0.0).astype(BF16)

    def normalize(raw, tangent, own, other):
        x = raw.astype(F32)
        u = tangent.astype(F32)
        inverse = lax.rsqrt(jnp.mean(x * x, axis=1, keepdims=True) + EPSILON)
        coupling = jnp.mean(x * u, axis=1, keepdims=True)
        x_turned = x * own + jnp.dot(raw, exchange, preferred_element_type=F32) * other
        u_turned = u * own + jnp.dot(tangent, exchange, preferred_element_type=F32) * other
        dotted = u_turned * inverse - x_turned * (inverse * inverse * inverse * coupling)
        return x_turned * inverse, dotted

    idle = 2 * HEADS * SEND
    out[idle:, :] = jnp.zeros((CHIPS * SEND - idle, HD), BF16)
    for copy in copies:
        copy.wait()
    of_query = turned(query_gain[...])
    of_key = turned(key_gain[...])
    for head in range(HEADS):
        here = lanes(head)
        q_hat, q_dot = normalize(query[:, here], query_t[:, here], *of_query)
        k_hat, k_dot = normalize(key[:, here], key_t[:, here], *of_key)
        parts = (k_hat.astype(BF16), k_dot.astype(BF16), value[:, here], value_t[:, here])
        for half in range(2):
            at = chip_of(head, half) * SEND
            for t, part in enumerate(parts):
                out[at + LOCAL * t : at + LOCAL * t + LOCAL, :] = part
            ours = slice(HALF * half, HALF * half + HALF)
            queries = jnp.concatenate([q_hat[ours], q_dot[ours]], axis=0)
            out[at + 4 * LOCAL : at + SEND, :] = queries.astype(BF16)


def repack_keys(received, keys):
    for source in range(CHIPS):
        at = source * SEND
        for t in range(4):
            keys[LOCAL * source : LOCAL * source + LOCAL, HD * t : HD * t + HD] = received[
                at + LOCAL * t : at + LOCAL * t + LOCAL, :
            ]


def repack_queries(received, query_pair):
    for source in range(0, CHIPS, 2):
        two = [received[s * SEND + 4 * LOCAL : s * SEND + SEND, :].astype(F32) for s in (source, source + 1)]
        rows = slice(HALF * source, HALF * source + LOCAL)
        query_pair[rows, HD:] = jnp.concatenate([part[:HALF] for part in two], axis=0).astype(BF16)
        query_pair[rows, :HD] = jnp.concatenate([part[HALF:] for part in two], axis=0).astype(BF16)


TRANSPOSED = (((1,), (1,)), ((), ()))
BQ = 576


def absorb(query_pair, blocks, at, state):
    pair = query_pair[at, :]
    hat = query_pair[at, HD:]
    scores = [lax.dot_general(hat, kv[:, 0:HD], TRANSPOSED, preferred_element_type=F32) for kv in blocks]
    peak = None if state is None else state[0]
    for s in scores:
        top = jnp.max(s, axis=1, keepdims=True)
        peak = top if peak is None else jnp.maximum(peak, top)
    total = drift = both = extra = 0.0
    for s, kv in zip(scores, blocks):
        weights = jnp.exp2((s - peak) * (SCALE * math.log2(math.e)))
        moved = lax.dot_general(pair, kv[:, 0 : 2 * HD], TRANSPOSED, preferred_element_type=F32)
        product = weights * (moved * SCALE)
        total = total + jnp.sum(weights, axis=1, keepdims=True)
        drift = drift + jnp.sum(product, axis=1, keepdims=True)
        both = both + jnp.dot(weights.astype(BF16), kv[:, 2 * HD : 4 * HD], preferred_element_type=F32)
        extra = extra + jnp.dot(product.astype(BF16), kv[:, 2 * HD : 3 * HD], preferred_element_type=F32)
    summed = both[:, :HD]
    summed_dot = both[:, HD:] + extra
    if state is None:
        return peak, total, drift, summed, summed_dot
    rescale = jnp.exp2((state[0] - peak) * (SCALE * math.log2(math.e)))
    old = [part * rescale for part in state[1:]]
    return peak, old[0] + total, old[1] + drift, old[2] + summed, old[3] + summed_dot


QUERY_BLOCKS = [slice(b, b + BQ) for b in range(0, QUERIES, BQ)]


def attend_first(received, query_pair, *rest):
    state, keys = rest[:-1], rest[-1]
    repack_queries(received, query_pair)
    repack_keys(received, keys)
    for at in QUERY_BLOCKS:
        for ref, part in zip(state, absorb(query_pair, (keys,), at, None)):
            ref[at, :] = part


def attend_last(query_pair, received, *rest):
    before, (out, kv, attended, attended_t) = rest[:5], rest[5:]
    repack_keys(received, kv)
    for at in QUERY_BLOCKS:
        state = absorb(query_pair, (kv,), at, [ref[at, :] for ref in before])
        _, total, drift, summed, summed_dot = state
        attended[at, :] = summed / total
        attended_t[at, :] = (summed_dot - drift / total * summed) / total
    for source in range(CHIPS):
        rows = slice(HALF * source, HALF * source + HALF)
        both = jnp.concatenate([attended[rows, :], attended_t[rows, :]], axis=0)
        out[BACK * source : BACK * source + BACK, :] = both.astype(BF16)


def unpack(received, attended, attended_t):
    for head in range(HEADS):
        halves = []
        for half in range(2):
            at = chip_of(head, half) * BACK
            halves.append(received[at : at + BACK, :].astype(F32))
        here = lanes(head)
        attended[:, here] = jnp.concatenate([part[:HALF] for part in halves], axis=0).astype(BF16)
        attended_t[:, here] = jnp.concatenate([part[HALF:] for part in halves], axis=0).astype(BF16)


def call(kernel, outs, scratch=(), specs=None, kept=True, keys=0):
    make = pltpu.VMEM if kept else jax.ShapeDtypeStruct
    shapes = tuple(make(shape, dtype) for shape, dtype in outs)
    one = len(shapes) == 1

    def run(*args):
        places = specs or [VMEM] * len(args)
        args = [
            a if spec is SMEM else pltpu.with_memory_space_constraint(a, spec.memory_space)
            for a, spec in zip(args, places)
        ]
        return pl.pallas_call(
            kernel,
            out_shape=shapes[0] if one else shapes,
            in_specs=places,
            out_specs=VMEM if one else (VMEM,) * len(shapes),
            scratch_shapes=list(scratch),
            cost_estimate=pl.CostEstimate(
                flops=16 * QUERIES * HD * keys, transcendentals=QUERIES * keys, bytes_accessed=10**6
            ),
            compiler_params=pltpu.CompilerParams(vmem_limit_bytes=24 * 2**20),
            name=kernel.__name__,
        )(*args)

    return run


def exchanged(message, rows):
    pairs = message.reshape(CHIPS, rows // 2, 2, HD)
    pairs = lax.all_to_all(pairs, ("yhi", "z", "ylo"), 0, 0, tiled=True)
    return pairs.reshape(CHIPS * rows, HD)


def local(query, key, value, query_t, key_t, value_t, query_gain, key_gain):
    place = lax.axis_index("z") * 2 + lax.axis_index("ylo")
    share = lax.axis_index("yhi") * 2 + lax.axis_index("core")
    first = (place * ROWS + share * LOCAL).reshape(1)
    rows = [a.reshape(LOCAL, D) for a in (query, key, value, query_t, key_t, value_t)]
    landing = [pltpu.VMEM((LOCAL, D), BF16)] * 6 + [pltpu.VMEM((1, HD), F32)] * 2
    landing.append(pltpu.SemaphoreType.DMA((8,)))
    message = call(
        prepare,
        [((CHIPS * SEND, HD), BF16)],
        landing,
        specs=[SMEM] + [HBM] * 8,
    )(first, *rows, query_gain.reshape(1, HD), key_gain.reshape(1, HD))
    received = exchanged(message, SEND)
    beside = lax.ppermute(received, "core", [(0, 1), (1, 0)])
    state_shapes = [((QUERIES, 1), F32)] * 3 + [((QUERIES, HD), F32)] * 2
    keys = pltpu.VMEM((KEYS, 4 * HD), BF16)
    query_pair, *state = call(attend_first, [((QUERIES, 2 * HD), BF16)] + state_shapes, [keys], keys=KEYS)(received)
    message = call(
        attend_last,
        [((CHIPS * BACK, HD), BF16)],
        [keys] + [pltpu.VMEM((QUERIES, HD), F32)] * 2,
        keys=KEYS,
    )(query_pair, beside, *state)
    received = exchanged(message, BACK)
    attended, attended_t = call(unpack, [((LOCAL, D), BF16)] * 2, kept=False)(received)
    return attended.reshape(1, LOCAL, D), attended_t.reshape(1, LOCAL, D)


def solution(mesh):
    fine = Mesh(mesh.devices.reshape(4, 2, 8, 2, 4), ("yhi", "core", "z", "ylo", "x"))
    spec = P(("z", "ylo", "x"), ("yhi", "core"), None)
    return jax.shard_map(
        local,
        mesh=fine,
        in_specs=(spec,) * 6 + (P(), P()),
        out_specs=(spec, spec),
        check_vma=False,
    )
```

```python
import math

import jax
import jax.numpy as jnp
from jax import lax
from jax.experimental import pallas as pl
from jax.experimental.pallas import tpu as pltpu
from jax.sharding import Mesh
from jax.sharding import PartitionSpec as P

HEADS = 24
HD = 128
D = 3072
TXT = 512
GRID_W = 64
ROWS = 144
LOCAL = 18
CHIPS = 64
KEYS = 1152
QUERIES = 576
HALF = 9
SEND = 90
BACK = 18
EPSILON = 1e-06
THETA = 10000.0
SCALE = 1.0 / math.sqrt(HD)
F32 = jnp.float32
BF16 = jnp.bfloat16

VMEM = pl.BlockSpec(memory_space=pltpu.VMEM)
SMEM = pl.BlockSpec(memory_space=pltpu.SMEM)
HBM = pl.BlockSpec(memory_space=pltpu.HBM)


def chip_of(head, half):
    return (head % 3) * 16 + head // 3 * 2 + half


def lanes(head):
    return slice(head * HD, (head + 1) * HD)


def prepare(first, *refs):
    sources, out, buffers, arrival = refs[:8], refs[8], refs[9:17], refs[17]
    copies = [
        pltpu.make_async_copy(source, buffer, arrival.at[i])
        for i, (source, buffer) in enumerate(zip(sources, buffers))
    ]
    for copy in copies:
        copy.start()
    query, key, value, query_t, key_t, value_t, query_gain, key_gain = buffers
    token = first[0] + lax.broadcasted_iota(jnp.int32, (LOCAL, HD), 0)
    lane = lax.broadcasted_iota(jnp.int32, (LOCAL, HD), 1)
    patch = jnp.maximum(token - TXT, 0)
    is_image = token >= TXT
    row_id = jnp.where(is_image, lax.shift_right_logical(patch, 6), 0).astype(F32)
    column_id = jnp.where(is_image, patch & (GRID_W - 1), 0).astype(F32)
    pair = lax.shift_right_logical(lane, 1)
    of_row = pair < 36
    step = jnp.where(of_row, pair - 8, pair - 36).astype(F32)
    frequency = jnp.exp(-math.log(THETA) * (step * (2.0 / 56.0)))
    angle = jnp.where(pair < 8, 0.0, jnp.where(of_row, row_id, column_id) * frequency)
    cosine = jnp.cos(angle)
    even = (lane & 1) == 0
    sine = jnp.where(even, -jnp.sin(angle), jnp.sin(angle))

    def turned(gain):
        wide = jnp.broadcast_to(gain, (LOCAL, HD))
        partner = jnp.where(even, pltpu.roll(wide, HD - 1, 1), pltpu.roll(wide, 1, 1))
        return wide * cosine, partner * sine

    row = lax.broadcasted_iota(jnp.int32, (HD, HD), 0)
    column = lax.broadcasted_iota(jnp.int32, (HD, HD), 1)
    exchange = jnp.where((row ^ 1) == column, 1.0, 0.0).astype(BF16)

    def normalize(raw, tangent, own, other):
        x = raw.astype(F32)
        u = tangent.astype(F32)
        inverse = lax.rsqrt(jnp.mean(x * x, axis=1, keepdims=True) + EPSILON)
        coupling = jnp.mean(x * u, axis=1, keepdims=True)
        x_turned = x * own + jnp.dot(raw, exchange, preferred_element_type=F32) * other
        u_turned = u * own + jnp.dot(tangent, exchange, preferred_element_type=F32) * other
        dotted = u_turned * inverse - x_turned * (inverse * inverse * inverse * coupling)
        return x_turned * inverse, dotted

    idle = 2 * HEADS * SEND
    out[idle:, :] = jnp.zeros((CHIPS * SEND - idle, HD), BF16)
    for copy in copies:
        copy.wait()
    of_query = turned(query_gain[...])
    of_key = turned(key_gain[...])
    for head in range(HEADS):
        here = lanes(head)
        q_hat, q_dot = normalize(query[:, here], query_t[:, here], *of_query)
        k_hat, k_dot = normalize(key[:, here], key_t[:, here], *of_key)
        parts = (k_hat.astype(BF16), k_dot.astype(BF16), value[:, here], value_t[:, here])
        for half in range(2):
            at = chip_of(head, half) * SEND
            for t, part in enumerate(parts):
                out[at + LOCAL * t : at + LOCAL * t + LOCAL, :] = part
            ours = slice(HALF * half, HALF * half + HALF)
            queries = jnp.concatenate([q_hat[ours], q_dot[ours]], axis=0)
            out[at + 4 * LOCAL : at + SEND, :] = queries.astype(BF16)


def repack_keys(received, keys):
    for source in range(CHIPS):
        at = source * SEND
        for t in range(4):
            keys[LOCAL * source : LOCAL * source + LOCAL, HD * t : HD * t + HD] = received[
                at + LOCAL * t : at + LOCAL * t + LOCAL, :
            ]


def repack_queries(received, query_pair):
    for source in range(0, CHIPS, 2):
        two = [received[s * SEND + 4 * LOCAL : s * SEND + SEND, :].astype(F32) for s in (source, source + 1)]
        rows = slice(HALF * source, HALF * source + LOCAL)
        query_pair[rows, HD:] = jnp.concatenate([part[:HALF] for part in two], axis=0).astype(BF16)
        query_pair[rows, :HD] = jnp.concatenate([part[HALF:] for part in two], axis=0).astype(BF16)


TRANSPOSED = (((1,), (1,)), ((), ()))
BQ = 576


def absorb(query_pair, blocks, at, state):
    pair = query_pair[at, :]
    hat = query_pair[at, HD:]
    scores = [lax.dot_general(hat, kv[:, 0:HD], TRANSPOSED, preferred_element_type=F32) for kv in blocks]
    peak = None if state is None else state[0]
    for s in scores:
        top = jnp.max(s, axis=1, keepdims=True)
        peak = top if peak is None else jnp.maximum(peak, top)
    total = drift = both = extra = 0.0
    for s, kv in zip(scores, blocks):
        weights = jnp.exp2((s - peak) * (SCALE * math.log2(math.e)))
        moved = lax.dot_general(pair, kv[:, 0 : 2 * HD], TRANSPOSED, preferred_element_type=F32)
        product = weights * (moved * SCALE)
        total = total + jnp.sum(weights, axis=1, keepdims=True)
        drift = drift + jnp.sum(product, axis=1, keepdims=True)
        both = both + jnp.dot(weights.astype(BF16), kv[:, 2 * HD : 4 * HD], preferred_element_type=F32)
        extra = extra + jnp.dot(product.astype(BF16), kv[:, 2 * HD : 3 * HD], preferred_element_type=F32)
    summed = both[:, :HD]
    summed_dot = both[:, HD:] + extra
    if state is None:
        return peak, total, drift, summed, summed_dot
    rescale = jnp.exp2((state[0] - peak) * (SCALE * math.log2(math.e)))
    old = [part * rescale for part in state[1:]]
    return peak, old[0] + total, old[1] + drift, old[2] + summed, old[3] + summed_dot


QUERY_BLOCKS = [slice(b, b + BQ) for b in range(0, QUERIES, BQ)]


def attend_first(received, keys, query_pair, *state):
    repack_queries(received, query_pair)
    for at in QUERY_BLOCKS:
        for ref, part in zip(state, absorb(query_pair, (keys,), at, None)):
            ref[at, :] = part


def attend_last(query_pair, kv, *rest):
    before, (out, attended, attended_t) = rest[:5], rest[5:]
    for at in QUERY_BLOCKS:
        state = absorb(query_pair, (kv,), at, [ref[at, :] for ref in before])
        _, total, drift, summed, summed_dot = state
        attended[at, :] = summed / total
        attended_t[at, :] = (summed_dot - drift / total * summed) / total
    for source in range(CHIPS):
        rows = slice(HALF * source, HALF * source + HALF)
        both = jnp.concatenate([attended[rows, :], attended_t[rows, :]], axis=0)
        out[BACK * source : BACK * source + BACK, :] = both.astype(BF16)


def unpack(received, attended, attended_t):
    for head in range(HEADS):
        halves = []
        for half in range(2):
            at = chip_of(head, half) * BACK
            halves.append(received[at : at + BACK, :].astype(F32))
        here = lanes(head)
        attended[:, here] = jnp.concatenate([part[:HALF] for part in halves], axis=0).astype(BF16)
        attended_t[:, here] = jnp.concatenate([part[HALF:] for part in halves], axis=0).astype(BF16)


def call(kernel, outs, scratch=(), specs=None, kept=True, keys=0):
    make = pltpu.VMEM if kept else jax.ShapeDtypeStruct
    shapes = tuple(make(shape, dtype) for shape, dtype in outs)
    one = len(shapes) == 1

    def run(*args):
        places = specs or [VMEM] * len(args)
        args = [
            a if spec is SMEM else pltpu.with_memory_space_constraint(a, spec.memory_space)
            for a, spec in zip(args, places)
        ]
        return pl.pallas_call(
            kernel,
            out_shape=shapes[0] if one else shapes,
            in_specs=places,
            out_specs=VMEM if one else (VMEM,) * len(shapes),
            scratch_shapes=list(scratch),
            cost_estimate=pl.CostEstimate(
                flops=16 * QUERIES * HD * keys, transcendentals=QUERIES * keys, bytes_accessed=10**6
            ),
            compiler_params=pltpu.CompilerParams(vmem_limit_bytes=24 * 2**20),
            name=kernel.__name__,
        )(*args)

    return run


def exchanged(message, rows):
    pairs = message.reshape(CHIPS, rows // 2, 2, HD)
    pairs = lax.all_to_all(pairs, ("yhi", "z", "ylo"), 0, 0, tiled=True)
    return pairs.reshape(CHIPS * rows, HD)


def local(query, key, value, query_t, key_t, value_t, query_gain, key_gain):
    place = lax.axis_index("z") * 2 + lax.axis_index("ylo")
    share = lax.axis_index("yhi") * 2 + lax.axis_index("core")
    first = (place * ROWS + share * LOCAL).reshape(1)
    rows = [a.reshape(LOCAL, D) for a in (query, key, value, query_t, key_t, value_t)]
    landing = [pltpu.VMEM((LOCAL, D), BF16)] * 6 + [pltpu.VMEM((1, HD), F32)] * 2
    landing.append(pltpu.SemaphoreType.DMA((8,)))
    message = call(
        prepare,
        [((CHIPS * SEND, HD), BF16)],
        landing,
        specs=[SMEM] + [HBM] * 8,
    )(first, *rows, query_gain.reshape(1, HD), key_gain.reshape(1, HD))
    received = exchanged(message, SEND)
    keys = call(repack_keys, [((KEYS, 4 * HD), BF16)])(received)
    beside = lax.ppermute(keys, "core", [(0, 1), (1, 0)])
    state_shapes = [((QUERIES, 1), F32)] * 3 + [((QUERIES, HD), F32)] * 2
    query_pair, *state = call(attend_first, [((QUERIES, 2 * HD), BF16)] + state_shapes, keys=KEYS)(received, keys)
    message = call(
        attend_last, [((CHIPS * BACK, HD), BF16)], [pltpu.VMEM((QUERIES, HD), F32)] * 2, keys=KEYS
    )(query_pair, beside, *state)
    received = exchanged(message, BACK)
    attended, attended_t = call(unpack, [((LOCAL, D), BF16)] * 2, kept=False)(received)
    return attended.reshape(1, LOCAL, D), attended_t.reshape(1, LOCAL, D)


def solution(mesh):
    fine = Mesh(mesh.devices.reshape(4, 2, 8, 2, 4), ("yhi", "core", "z", "ylo", "x"))
    spec = P(("z", "ylo", "x"), ("yhi", "core"), None)
    return jax.shard_map(
        local,
        mesh=fine,
        in_specs=(spec,) * 6 + (P(), P()),
        out_specs=(spec, spec),
        check_vma=False,
    )
```

```python
import math

import jax
import jax.numpy as jnp
from jax import lax
from jax.experimental import pallas as pl
from jax.experimental.pallas import tpu as pltpu
from jax.sharding import Mesh
from jax.sharding import PartitionSpec as P

HEADS = 24
HD = 128
D = 3072
TXT = 512
GRID_W = 64
ROWS = 144
LOCAL = 18
CHIPS = 64
KEYS = 1152
QUERIES = 576
HALF = 9
SEND = 90
BACK = 18
EPSILON = 1e-06
THETA = 10000.0
SCALE = 1.0 / math.sqrt(HD)
F32 = jnp.float32
BF16 = jnp.bfloat16

VMEM = pl.BlockSpec(memory_space=pltpu.VMEM)
SMEM = pl.BlockSpec(memory_space=pltpu.SMEM)
HBM = pl.BlockSpec(memory_space=pltpu.HBM)


def chip_of(head, half):
    return (head % 3) * 16 + head // 3 * 2 + half


def lanes(head):
    return slice(head * HD, (head + 1) * HD)


def prepare(first, *refs):
    sources, out, buffers, arrival = refs[:8], refs[8], refs[9:17], refs[17]
    copies = [
        pltpu.make_async_copy(source, buffer, arrival.at[i])
        for i, (source, buffer) in enumerate(zip(sources, buffers))
    ]
    for i in (6, 7, 0, 3, 1, 4, 2, 5):
        copies[i].start()
    query, key, value, query_t, key_t, value_t, query_gain, key_gain = buffers
    token = first[0] + lax.broadcasted_iota(jnp.int32, (LOCAL, HD), 0)
    lane = lax.broadcasted_iota(jnp.int32, (LOCAL, HD), 1)
    patch = jnp.maximum(token - TXT, 0)
    is_image = token >= TXT
    row_id = jnp.where(is_image, lax.shift_right_logical(patch, 6), 0).astype(F32)
    column_id = jnp.where(is_image, patch & (GRID_W - 1), 0).astype(F32)
    pair = lax.shift_right_logical(lane, 1)
    of_row = pair < 36
    step = jnp.where(of_row, pair - 8, pair - 36).astype(F32)
    frequency = jnp.exp(-math.log(THETA) * (step * (2.0 / 56.0)))
    angle = jnp.where(pair < 8, 0.0, jnp.where(of_row, row_id, column_id) * frequency)
    cosine = jnp.cos(angle)
    even = (lane & 1) == 0
    sine = jnp.where(even, -jnp.sin(angle), jnp.sin(angle))

    def turned(gain):
        wide = jnp.broadcast_to(gain, (LOCAL, HD))
        partner = jnp.where(even, pltpu.roll(wide, HD - 1, 1), pltpu.roll(wide, 1, 1))
        return wide * cosine, partner * sine

    row = lax.broadcasted_iota(jnp.int32, (HD, HD), 0)
    column = lax.broadcasted_iota(jnp.int32, (HD, HD), 1)
    exchange = jnp.where((row ^ 1) == column, 1.0, 0.0).astype(BF16)

    def normalize(raw, tangent, own, other):
        x = raw.astype(F32)
        u = tangent.astype(F32)
        inverse = lax.rsqrt(jnp.mean(x * x, axis=1, keepdims=True) + EPSILON)
        coupling = jnp.mean(x * u, axis=1, keepdims=True)
        x_turned = x * own + jnp.dot(raw, exchange, preferred_element_type=F32) * other
        u_turned = u * own + jnp.dot(tangent, exchange, preferred_element_type=F32) * other
        dotted = u_turned * inverse - x_turned * (inverse * inverse * inverse * coupling)
        return x_turned * inverse, dotted

    idle = 2 * HEADS * SEND
    out[idle:, :] = jnp.zeros((CHIPS * SEND - idle, HD), BF16)
    for i in (6, 7, 0, 3):
        copies[i].wait()
    of_query = turned(query_gain[...])
    of_key = turned(key_gain[...])
    for head in range(HEADS):
        here = lanes(head)
        q_hat, q_dot = normalize(query[:, here], query_t[:, here], *of_query)
        for half in range(2):
            at = chip_of(head, half) * SEND
            ours = slice(HALF * half, HALF * half + HALF)
            queries = jnp.concatenate([q_hat[ours], q_dot[ours]], axis=0)
            out[at + 4 * LOCAL : at + SEND, :] = queries.astype(BF16)
    for i in (1, 4, 2, 5):
        copies[i].wait()
    for head in range(HEADS):
        here = lanes(head)
        k_hat, k_dot = normalize(key[:, here], key_t[:, here], *of_key)
        parts = (k_hat.astype(BF16), k_dot.astype(BF16), value[:, here], value_t[:, here])
        for half in range(2):
            at = chip_of(head, half) * SEND
            for t, part in enumerate(parts):
                out[at + LOCAL * t : at + LOCAL * t + LOCAL, :] = part


def repack_keys(received, keys):
    for source in range(CHIPS):
        at = source * SEND
        for t in range(4):
            keys[LOCAL * source : LOCAL * source + LOCAL, HD * t : HD * t + HD] = received[
                at + LOCAL * t : at + LOCAL * t + LOCAL, :
            ]


def repack_queries(received, query_pair):
    for source in range(0, CHIPS, 2):
        two = [received[s * SEND + 4 * LOCAL : s * SEND + SEND, :].astype(F32) for s in (source, source + 1)]
        rows = slice(HALF * source, HALF * source + LOCAL)
        query_pair[rows, HD:] = jnp.concatenate([part[:HALF] for part in two], axis=0).astype(BF16)
        query_pair[rows, :HD] = jnp.concatenate([part[HALF:] for part in two], axis=0).astype(BF16)


TRANSPOSED = (((1,), (1,)), ((), ()))
BQ = 576


def absorb(query_pair, blocks, at, state):
    pair = query_pair[at, :]
    hat = query_pair[at, HD:]
    scores = [lax.dot_general(hat, kv[:, 0:HD], TRANSPOSED, preferred_element_type=F32) for kv in blocks]
    peak = None if state is None else state[0]
    for s in scores:
        top = jnp.max(s, axis=1, keepdims=True)
        peak = top if peak is None else jnp.maximum(peak, top)
    total = drift = both = extra = 0.0
    for s, kv in zip(scores, blocks):
        weights = jnp.exp2((s - peak) * (SCALE * math.log2(math.e)))
        moved = lax.dot_general(pair, kv[:, 0 : 2 * HD], TRANSPOSED, preferred_element_type=F32)
        product = weights * moved
        total = total + jnp.sum(weights, axis=1, keepdims=True)
        drift = drift + jnp.sum(product, axis=1, keepdims=True)
        both = both + jnp.dot(weights.astype(BF16), kv[:, 2 * HD : 4 * HD], preferred_element_type=F32)
        extra = extra + jnp.dot(product.astype(BF16), kv[:, 2 * HD : 3 * HD], preferred_element_type=F32)
    drift = drift * SCALE
    summed = both[:, :HD]
    summed_dot = both[:, HD:] + extra * SCALE
    if state is None:
        return peak, total, drift, summed, summed_dot
    rescale = jnp.exp2((state[0] - peak) * (SCALE * math.log2(math.e)))
    old = [part * rescale for part in state[1:]]
    return peak, old[0] + total, old[1] + drift, old[2] + summed, old[3] + summed_dot


QUERY_BLOCKS = [slice(b, b + BQ) for b in range(0, QUERIES, BQ)]


def attend_first(received, keys, query_pair, *state):
    repack_queries(received, query_pair)
    for at in QUERY_BLOCKS:
        for ref, part in zip(state, absorb(query_pair, (keys,), at, None)):
            ref[at, :] = part


def attend_last(query_pair, kv, *rest):
    before, (out, attended, attended_t) = rest[:5], rest[5:]
    for at in QUERY_BLOCKS:
        state = absorb(query_pair, (kv,), at, [ref[at, :] for ref in before])
        _, total, drift, summed, summed_dot = state
        attended[at, :] = summed / total
        attended_t[at, :] = (summed_dot - drift / total * summed) / total
    for source in range(CHIPS):
        rows = slice(HALF * source, HALF * source + HALF)
        both = jnp.concatenate([attended[rows, :], attended_t[rows, :]], axis=0)
        out[BACK * source : BACK * source + BACK, :] = both.astype(BF16)


def unpack(received, attended, attended_t):
    for head in range(HEADS):
        halves = []
        for half in range(2):
            at = chip_of(head, half) * BACK
            halves.append(received[at : at + BACK, :].astype(F32))
        here = lanes(head)
        attended[:, here] = jnp.concatenate([part[:HALF] for part in halves], axis=0).astype(BF16)
        attended_t[:, here] = jnp.concatenate([part[HALF:] for part in halves], axis=0).astype(BF16)


def call(kernel, outs, scratch=(), specs=None, kept=True, keys=0):
    make = pltpu.VMEM if kept else jax.ShapeDtypeStruct
    shapes = tuple(make(shape, dtype) for shape, dtype in outs)
    one = len(shapes) == 1

    def run(*args):
        places = specs or [VMEM] * len(args)
        args = [
            a if spec is SMEM else pltpu.with_memory_space_constraint(a, spec.memory_space)
            for a, spec in zip(args, places)
        ]
        return pl.pallas_call(
            kernel,
            out_shape=shapes[0] if one else shapes,
            in_specs=places,
            out_specs=VMEM if one else (VMEM,) * len(shapes),
            scratch_shapes=list(scratch),
            cost_estimate=pl.CostEstimate(
                flops=16 * QUERIES * HD * keys, transcendentals=QUERIES * keys, bytes_accessed=10**6
            ),
            compiler_params=pltpu.CompilerParams(vmem_limit_bytes=24 * 2**20),
            name=kernel.__name__,
        )(*args)

    return run


def exchanged(message, rows):
    pairs = message.reshape(CHIPS, rows // 2, 2, HD)
    pairs = lax.all_to_all(pairs, ("yhi", "z", "ylo"), 0, 0, tiled=True)
    return pairs.reshape(CHIPS * rows, HD)


def local(query, key, value, query_t, key_t, value_t, query_gain, key_gain):
    place = lax.axis_index("z") * 2 + lax.axis_index("ylo")
    share = lax.axis_index("yhi") * 2 + lax.axis_index("core")
    first = (place * ROWS + share * LOCAL).reshape(1)
    rows = [a.reshape(LOCAL, D) for a in (query, key, value, query_t, key_t, value_t)]
    landing = [pltpu.VMEM((LOCAL, D), BF16)] * 6 + [pltpu.VMEM((1, HD), F32)] * 2
    landing.append(pltpu.SemaphoreType.DMA((8,)))
    message = call(
        prepare,
        [((CHIPS * SEND, HD), BF16)],
        landing,
        specs=[SMEM] + [HBM] * 8,
    )(first, *rows, query_gain.reshape(1, HD), key_gain.reshape(1, HD))
    received = exchanged(message, SEND)
    keys = call(repack_keys, [((KEYS, 4 * HD), BF16)])(received)
    beside = lax.ppermute(keys, "core", [(0, 1), (1, 0)])
    state_shapes = [((QUERIES, 1), F32)] * 3 + [((QUERIES, HD), F32)] * 2
    query_pair, *state = call(attend_first, [((QUERIES, 2 * HD), BF16)] + state_shapes, keys=KEYS)(received, keys)
    message = call(
        attend_last, [((CHIPS * BACK, HD), BF16)], [pltpu.VMEM((QUERIES, HD), F32)] * 2, keys=KEYS
    )(query_pair, beside, *state)
    received = exchanged(message, BACK)
    attended, attended_t = call(unpack, [((LOCAL, D), BF16)] * 2, kept=False)(received)
    return attended.reshape(1, LOCAL, D), attended_t.reshape(1, LOCAL, D)


def solution(mesh):
    fine = Mesh(mesh.devices.reshape(4, 2, 8, 2, 4), ("yhi", "core", "z", "ylo", "x"))
    spec = P(("z", "ylo", "x"), ("yhi", "core"), None)
    return jax.shard_map(
        local,
        mesh=fine,
        in_specs=(spec,) * 6 + (P(), P()),
        out_specs=(spec, spec),
        check_vma=False,
    )
```

```python
import math

import jax
import jax.numpy as jnp
from jax import lax
from jax.experimental import pallas as pl
from jax.experimental.pallas import tpu as pltpu
from jax.sharding import Mesh
from jax.sharding import PartitionSpec as P

HEADS = 24
HD = 128
D = 3072
TXT = 512
GRID_W = 64
ROWS = 144
LOCAL = 18
CHIPS = 64
KEYS = 1152
QUERIES = 576
HALF = 9
SEND = 90
BACK = 18
EPSILON = 1e-06
THETA = 10000.0
SCALE = 1.0 / math.sqrt(HD)
F32 = jnp.float32
BF16 = jnp.bfloat16

VMEM = pl.BlockSpec(memory_space=pltpu.VMEM)
SMEM = pl.BlockSpec(memory_space=pltpu.SMEM)
HBM = pl.BlockSpec(memory_space=pltpu.HBM)


def chip_of(head, half):
    return (head % 3) * 16 + head // 3 * 2 + half


def lanes(head):
    return slice(head * HD, (head + 1) * HD)


def prepare(first, *refs):
    sources, out, buffers, arrival = refs[:8], refs[8], refs[9:17], refs[17]
    copies = [
        pltpu.make_async_copy(source, buffer, arrival.at[i])
        for i, (source, buffer) in enumerate(zip(sources, buffers))
    ]
    for i in (6, 7, 0, 3, 1, 4, 2, 5):
        copies[i].start()
    query, key, value, query_t, key_t, value_t, query_gain, key_gain = buffers
    token = first[0] + lax.broadcasted_iota(jnp.int32, (LOCAL, HD), 0)
    lane = lax.broadcasted_iota(jnp.int32, (LOCAL, HD), 1)
    patch = jnp.maximum(token - TXT, 0)
    is_image = token >= TXT
    row_id = jnp.where(is_image, lax.shift_right_logical(patch, 6), 0).astype(F32)
    column_id = jnp.where(is_image, patch & (GRID_W - 1), 0).astype(F32)
    pair = lax.shift_right_logical(lane, 1)
    of_row = pair < 36
    step = jnp.where(of_row, pair - 8, pair - 36).astype(F32)
    frequency = jnp.exp(-math.log(THETA) * (step * (2.0 / 56.0)))
    angle = jnp.where(pair < 8, 0.0, jnp.where(of_row, row_id, column_id) * frequency)
    cosine = jnp.cos(angle)
    even = (lane & 1) == 0
    sine = jnp.sin(jnp.where(even, -angle, angle))

    def turned(gain):
        wide = jnp.broadcast_to(gain, (LOCAL, HD))
        partner = jnp.where(even, pltpu.roll(wide, HD - 1, 1), pltpu.roll(wide, 1, 1))
        return wide * cosine, partner * sine

    row = lax.broadcasted_iota(jnp.int32, (HD, HD), 0)
    column = lax.broadcasted_iota(jnp.int32, (HD, HD), 1)
    exchange = jnp.where((row ^ 1) == column, 1.0, 0.0).astype(BF16)

    def normalize(raw, tangent, own, other):
        x = raw.astype(F32)
        u = tangent.astype(F32)
        inverse = lax.rsqrt(jnp.mean(x * x, axis=1, keepdims=True) + EPSILON)
        coupling = jnp.mean(x * u, axis=1, keepdims=True)
        x_turned = x * own + jnp.dot(raw, exchange, preferred_element_type=F32) * other
        u_turned = u * own + jnp.dot(tangent, exchange, preferred_element_type=F32) * other
        dotted = u_turned * inverse - x_turned * (inverse * inverse * inverse * coupling)
        return x_turned * inverse, dotted

    idle = 2 * HEADS * SEND
    out[idle:, :] = jnp.zeros((CHIPS * SEND - idle, HD), BF16)
    for i in (6, 7, 0, 3):
        copies[i].wait()
    of_query = turned(query_gain[...])
    of_key = turned(key_gain[...])
    for head in range(HEADS):
        here = lanes(head)
        q_hat, q_dot = normalize(query[:, here], query_t[:, here], *of_query)
        for half in range(2):
            at = chip_of(head, half) * SEND
            ours = slice(HALF * half, HALF * half + HALF)
            queries = jnp.concatenate([q_hat[ours], q_dot[ours]], axis=0)
            out[at + 4 * LOCAL : at + SEND, :] = queries.astype(BF16)
    for i in (1, 4):
        copies[i].wait()
    for head in range(HEADS):
        here = lanes(head)
        keys = normalize(key[:, here], key_t[:, here], *of_key)
        for half in range(2):
            at = chip_of(head, half) * SEND
            for t, part in enumerate(keys):
                out[at + LOCAL * t : at + LOCAL * t + LOCAL, :] = part.astype(BF16)
    for i in (2, 5):
        copies[i].wait()
    for head in range(HEADS):
        here = lanes(head)
        for half in range(2):
            at = chip_of(head, half) * SEND
            for t, part in enumerate((value[:, here], value_t[:, here]), 2):
                out[at + LOCAL * t : at + LOCAL * t + LOCAL, :] = part


def repack_keys(received, keys):
    for source in range(CHIPS):
        at = source * SEND
        for t in range(4):
            keys[LOCAL * source : LOCAL * source + LOCAL, HD * t : HD * t + HD] = received[
                at + LOCAL * t : at + LOCAL * t + LOCAL, :
            ]


def repack_queries(received, query_pair):
    for source in range(0, CHIPS, 2):
        two = [received[s * SEND + 4 * LOCAL : s * SEND + SEND, :].astype(F32) for s in (source, source + 1)]
        rows = slice(HALF * source, HALF * source + LOCAL)
        query_pair[rows, HD:] = jnp.concatenate([part[:HALF] for part in two], axis=0).astype(BF16)
        query_pair[rows, :HD] = jnp.concatenate([part[HALF:] for part in two], axis=0).astype(BF16)


TRANSPOSED = (((1,), (1,)), ((), ()))
BQ = 576


def absorb(query_pair, blocks, at, state):
    pair = query_pair[at, :]
    hat = query_pair[at, HD:]
    scores = [lax.dot_general(hat, kv[:, 0:HD], TRANSPOSED, preferred_element_type=F32) for kv in blocks]
    peak = None if state is None else state[0]
    for s in scores:
        top = jnp.max(s, axis=1, keepdims=True)
        peak = top if peak is None else jnp.maximum(peak, top)
    total = drift = both = extra = 0.0
    for s, kv in zip(scores, blocks):
        weights = jnp.exp2((s - peak) * (SCALE * math.log2(math.e)))
        moved = lax.dot_general(pair, kv[:, 0 : 2 * HD], TRANSPOSED, preferred_element_type=F32)
        product = weights * (moved * SCALE)
        total = total + jnp.sum(weights, axis=1, keepdims=True)
        drift = drift + jnp.sum(product, axis=1, keepdims=True)
        both = both + jnp.dot(weights.astype(BF16), kv[:, 2 * HD : 4 * HD], preferred_element_type=F32)
        extra = extra + jnp.dot(product.astype(BF16), kv[:, 2 * HD : 3 * HD], preferred_element_type=F32)
    summed = both[:, :HD]
    summed_dot = both[:, HD:] + extra
    if state is None:
        return peak, total, drift, summed, summed_dot
    rescale = jnp.exp2((state[0] - peak) * (SCALE * math.log2(math.e)))
    old = [part * rescale for part in state[1:]]
    return peak, old[0] + total, old[1] + drift, old[2] + summed, old[3] + summed_dot


QUERY_BLOCKS = [slice(b, b + BQ) for b in range(0, QUERIES, BQ)]


def attend_first(received, keys, query_pair, *state):
    repack_queries(received, query_pair)
    for at in QUERY_BLOCKS:
        for ref, part in zip(state, absorb(query_pair, (keys,), at, None)):
            ref[at, :] = part


def attend_last(query_pair, kv, *rest):
    before, (out, attended, attended_t) = rest[:5], rest[5:]
    for at in QUERY_BLOCKS:
        state = absorb(query_pair, (kv,), at, [ref[at, :] for ref in before])
        _, total, drift, summed, summed_dot = state
        attended[at, :] = summed / total
        attended_t[at, :] = (summed_dot - drift / total * summed) / total
    for source in range(CHIPS):
        rows = slice(HALF * source, HALF * source + HALF)
        both = jnp.concatenate([attended[rows, :], attended_t[rows, :]], axis=0)
        out[BACK * source : BACK * source + BACK, :] = both.astype(BF16)


def unpack(received, attended, attended_t):
    for head in range(HEADS):
        halves = []
        for half in range(2):
            at = chip_of(head, half) * BACK
            halves.append(received[at : at + BACK, :].astype(F32))
        here = lanes(head)
        attended[:, here] = jnp.concatenate([part[:HALF] for part in halves], axis=0).astype(BF16)
        attended_t[:, here] = jnp.concatenate([part[HALF:] for part in halves], axis=0).astype(BF16)


def call(kernel, outs, scratch=(), specs=None, kept=True, keys=0):
    make = pltpu.VMEM if kept else jax.ShapeDtypeStruct
    shapes = tuple(make(shape, dtype) for shape, dtype in outs)
    one = len(shapes) == 1

    def run(*args):
        places = specs or [VMEM] * len(args)
        args = [
            a if spec is SMEM else pltpu.with_memory_space_constraint(a, spec.memory_space)
            for a, spec in zip(args, places)
        ]
        return pl.pallas_call(
            kernel,
            out_shape=shapes[0] if one else shapes,
            in_specs=places,
            out_specs=VMEM if one else (VMEM,) * len(shapes),
            scratch_shapes=list(scratch),
            cost_estimate=pl.CostEstimate(
                flops=16 * QUERIES * HD * keys, transcendentals=QUERIES * keys, bytes_accessed=10**6
            ),
            compiler_params=pltpu.CompilerParams(vmem_limit_bytes=24 * 2**20),
            name=kernel.__name__,
        )(*args)

    return run


def exchanged(message, rows):
    pairs = message.reshape(CHIPS, rows // 2, 2, HD)
    pairs = lax.all_to_all(pairs, ("yhi", "z", "ylo"), 0, 0, tiled=True)
    return pairs.reshape(CHIPS * rows, HD)


def local(query, key, value, query_t, key_t, value_t, query_gain, key_gain):
    place = lax.axis_index("z") * 2 + lax.axis_index("ylo")
    share = lax.axis_index("yhi") * 2 + lax.axis_index("core")
    first = (place * ROWS + share * LOCAL).reshape(1)
    rows = [a.reshape(LOCAL, D) for a in (query, key, value, query_t, key_t, value_t)]
    landing = [pltpu.VMEM((LOCAL, D), BF16)] * 6 + [pltpu.VMEM((1, HD), F32)] * 2
    landing.append(pltpu.SemaphoreType.DMA((8,)))
    message = call(
        prepare,
        [((CHIPS * SEND, HD), BF16)],
        landing,
        specs=[SMEM] + [HBM] * 8,
    )(first, *rows, query_gain.reshape(1, HD), key_gain.reshape(1, HD))
    received = exchanged(message, SEND)
    keys = call(repack_keys, [((KEYS, 4 * HD), BF16)])(received)
    beside = lax.ppermute(keys, "core", [(0, 1), (1, 0)])
    state_shapes = [((QUERIES, 1), F32)] * 3 + [((QUERIES, HD), F32)] * 2
    query_pair, *state = call(attend_first, [((QUERIES, 2 * HD), BF16)] + state_shapes, keys=KEYS)(received, keys)
    message = call(
        attend_last, [((CHIPS * BACK, HD), BF16)], [pltpu.VMEM((QUERIES, HD), F32)] * 2, keys=KEYS
    )(query_pair, beside, *state)
    received = exchanged(message, BACK)
    attended, attended_t = call(unpack, [((LOCAL, D), BF16)] * 2, kept=False)(received)
    return attended.reshape(1, LOCAL, D), attended_t.reshape(1, LOCAL, D)


def solution(mesh):
    fine = Mesh(mesh.devices.reshape(4, 2, 8, 2, 4), ("yhi", "core", "z", "ylo", "x"))
    spec = P(("z", "ylo", "x"), ("yhi", "core"), None)
    return jax.shard_map(
        local,
        mesh=fine,
        in_specs=(spec,) * 6 + (P(), P()),
        out_specs=(spec, spec),
        check_vma=False,
    )
```
